32 devices in a mesh: shard: 2 (over x), replica: 16 (over z, y, core).
Axes of the slice: x: 2, y: 2, z: 4, core: 2. Of those that a mesh axis runs over, the one named last changes fastest.
Arguments:
- hidden_in: bfloat16 [16384, 2048], P(('shard', 'replica')), may hold values from -6 to 6
- out_cotangent: bfloat16 [16384, 2048], P(('shard', 'replica')), may hold values from -6 to 6
- segment_ids: int32 [16384], P(('shard', 'replica')), may hold values from 0 to 124, as said below
- ln1_gain: bfloat16 [2048], P('shard'), may hold values from 0.5 to 1.5
- ln1_bias: bfloat16 [2048], P('shard'), may hold values from -3 to 3
- qkv_weight: bfloat16 [2048, 6144], P('shard'), may hold values from -0.125 to 0.125
- qkv_bias: bfloat16 [6144], P('shard'), may hold values from -3 to 3
- dense_weight: bfloat16 [2048, 2048], P('shard'), may hold values from -0.375 to 0.375
- dense_bias: bfloat16 [2048], P('shard'), may hold values from -3 to 3
- ln2_gain: bfloat16 [2048], P('shard'), may hold values from 0.5 to 1.5
- ln2_bias: bfloat16 [2048], P('shard'), may hold values from -3 to 3
- fc1_weight: bfloat16 [2048, 4096], P('shard'), may hold values from -0.125 to 0.125
- fc1_bias: bfloat16 [4096], P('shard'), may hold values from -3 to 3
- fc2_weight: bfloat16 [4096, 2048], P('shard'), may hold values from -0.125 to 0.125
- fc2_bias: bfloat16 [2048], P('shard'), may hold values from -3 to 3
Outputs:
- hidden_out: bfloat16 [16384, 2048], P(('shard', 'replica'))
- grad_input: float32 [16384, 2048], P(('shard', 'replica'))
- grad_ln1_gain: float32 [2048], P(('shard', 'replica'))
- grad_ln1_bias: float32 [2048], P(('shard', 'replica'))
- grad_qkv_weight: float32 [2048, 6144], P(('shard', 'replica'))
- grad_qkv_bias: float32 [6144], P(('shard', 'replica'))
- grad_dense_weight: float32 [2048, 2048], P(('shard', 'replica'))
- grad_dense_bias: float32 [2048], P(('shard', 'replica'))
- grad_ln2_gain: float32 [2048], P(('shard', 'replica'))
- grad_ln2_bias: float32 [2048], P(('shard', 'replica'))
- grad_fc1_weight: float32 [2048, 4096], P(('shard', 'replica'))
- grad_fc1_bias: float32 [4096], P(('shard', 'replica'))
- grad_fc2_weight: float32 [4096, 2048], P(('shard', 'replica'))
- grad_fc2_bias: float32 [2048], P(('shard', 'replica'))
The draws below stay inside these ranges and needn't reach their ends.
Inputs may be any that keep to these rules, and one draw needn't show every extreme that they name: `segment_ids`: segment ids start at 0 and rise by one at each new sequence along the tokens; a segment lies within one aligned run of 512 tokens, so within one block of 512 tokens, and has at most 512 tokens; some block consists of segments of exactly 512 tokens.
All inputs are finite; a program needn't handle non-finite values.
Results may differ from the reference program's by a relative error of at most 0.0094.
Values may be sent and summed in bfloat16 or wider, within the bound.
A program may use at most 448 MiB of HBM per device.

```python
from functools import partial
import jax
import jax.numpy as jnp
from jax import lax

D = 2048
HEADS = 8
HEAD = 256
ROT = 64
FF = 4096
TOK_DEV = 512
TOKENS = 16384
SEQ_MAX = 512


def draw_segment_ids(key, part):
    runs = TOKENS // SEQ_MAX
    key_cut, key_dev = jax.random.split(jax.random.fold_in(key, 17))
    run_keys = jax.random.split(key_cut, runs)
    orders = jax.vmap(lambda one_key: jax.random.permutation(one_key, SEQ_MAX - 1))(run_keys).astype(jnp.int32)
    extra_cut = orders < 3
    quiet_block = jax.random.randint(key_dev, (), 0, TOKENS // TOK_DEV)
    run_block = jnp.arange(runs, dtype=jnp.int32) // (TOK_DEV // SEQ_MAX)
    active = (run_block != quiet_block)[:, None]
    inner = (extra_cut & active).astype(jnp.int32)
    heads = jnp.ones((runs, 1), jnp.int32)
    starts = jnp.concatenate([heads, inner], axis=1).reshape(TOKENS)
    return (jnp.cumsum(starts) - 1).astype(jnp.int32)


def level_of(stream_key, shape, pieces, smallest, high):
    gain, own = 1.0, jax.random.fold_in(stream_key, 6)
    for position, parts in pieces:
        heights = jnp.exp(jax.random.uniform(jax.random.fold_in(own, position), (parts,), jnp.float32, smallest / len(pieces), high / len(pieces)))
        gain = gain * jnp.repeat(heights, shape[position] // parts).reshape([-1 if axis == position else 1 for axis in range(len(shape))])
    return gain


def centred(own_key, shape, scale, most, cuts=(), held_as=jnp.bfloat16):
    values = jax.random.normal(own_key, shape, jnp.float32) * scale
    if len(cuts) > 0:
        values = level_of(own_key, shape, cuts, -0.22, 0.18) * values
    return jnp.clip(values, min=-most, max=most).astype(held_as)


def setup_inputs(seed: int = 0) -> dict:
    key_list = jax.random.split(jax.random.key(seed), 16)
    return {
        "hidden_in": centred(key_list[0], (TOKENS, D), 1.0, 6.0, ((0, 32),)),
        "out_cotangent": centred(key_list[1], (TOKENS, D), 1.0, 6.0, ((0, 32),)),
        "segment_ids": draw_segment_ids(jax.random.fold_in(key_list[15], 71), 0),
        "ln1_gain": jnp.clip(1.0 + 0.1 * jax.random.normal(key_list[3], (D,), jnp.float32), 0.5, 1.5).astype(jnp.bfloat16),
        "ln1_bias": centred(key_list[4], (D,), 0.3, 3.0, ((0, 2),)),
        "qkv_weight": centred(key_list[5], (D, 3 * D), D ** -0.5, 0.125, ((0, 2),)),
        "qkv_bias": centred(key_list[6], (3 * D,), 0.3, 3.0, ((0, 2),)),
        "dense_weight": centred(key_list[7], (D, D), (D // 8) ** -0.5, 0.375, ((0, 2),)),
        "dense_bias": centred(key_list[8], (D,), 0.3, 3.0, ((0, 2),)),
        "ln2_gain": jnp.clip(1.0 + 0.1 * jax.random.normal(key_list[9], (D,), jnp.float32), 0.5, 1.5).astype(jnp.bfloat16),
        "ln2_bias": centred(key_list[10], (D,), 0.3, 3.0, ((0, 2),)),
        "fc1_weight": centred(key_list[11], (D, FF), D ** -0.5, 0.125, ((0, 2),)),
        "fc1_bias": centred(key_list[12], (FF,), 0.5, 3.0, ((0, 2),)),
        "fc2_weight": centred(key_list[13], (FF, D), (FF // 2) ** -0.5, 0.125, ((0, 2),)),
        "fc2_bias": centred(key_list[14], (D,), 0.3, 3.0, ((0, 2),)),
    }


NEG_FILL = -1e+30
EPSILON = 1e-05

def layer_norm(values, gain_w, bias_w):
    center = values - lax.optimization_barrier(jnp.mean(values, axis=-1, keepdims=True))
    spread = lax.optimization_barrier(jnp.mean(center * center, axis=-1, keepdims=True))
    return center * lax.rsqrt(spread + EPSILON) * gain_w + bias_w

def rotary_angles(seg_row):
    row_count = seg_row.shape[0]
    row_index = jnp.arange(row_count, dtype=jnp.int32)
    same_seg = seg_row[:, None] == seg_row[None, :]
    first_pos = lax.optimization_barrier(jnp.min(jnp.where(same_seg, row_index[None, :], row_count), axis=1)).astype(jnp.int32)
    offset = (row_index - first_pos).astype(jnp.float32)
    frequency = jnp.exp(-jnp.log(10000.0) * jnp.arange(0, ROT, 2).astype(jnp.float32) / ROT)
    angles = offset[:, None] * frequency[None, :]
    allowed = same_seg & (row_index[None, :] <= row_index[:, None])
    return (jnp.cos(angles), jnp.sin(angles), allowed)

def rotate(heads_in, cos_table, sin_table):
    half_rot = ROT // 2
    part_one = heads_in[..., :half_rot]
    part_two = heads_in[..., half_rot:ROT]
    cos_b = cos_table[:, None, :]
    sin_b = sin_table[:, None, :]
    return jnp.concatenate([part_one * cos_b - part_two * sin_b, part_two * cos_b + part_one * sin_b, heads_in[..., ROT:]], axis=-1)

def gelu_exact(values):
    return 0.5 * values * (1.0 + lax.erf(values * 0.7071067811865476))

def masked_scores(query_b, keys_b, allowed):
    inv_root = query_b.shape[-1] ** (-0.5)
    scores = jnp.einsum('qhd,khd->hqk', query_b.astype(jnp.float32), keys_b.astype(jnp.float32)) * inv_root
    return jnp.where(allowed[None], scores, NEG_FILL)

def attention_forward(query_b, keys_b, vals_b, allowed):
    scores = masked_scores(query_b, keys_b, allowed)
    row_peak = lax.optimization_barrier(jnp.max(scores, axis=-1, keepdims=True))
    exp_terms = jnp.exp(scores - row_peak)
    row_total = lax.optimization_barrier(jnp.sum(exp_terms, axis=-1, keepdims=True))
    log_total = (row_peak + jnp.log(row_total))[..., 0]
    probs_b = (exp_terms / row_total).astype(jnp.bfloat16)
    context = jnp.einsum('hqk,khd->qhd', probs_b.astype(jnp.float32), vals_b.astype(jnp.float32))
    return (context, log_total)

def attention_backward(query_b, keys_b, vals_b, allowed, log_total, context, grad_ctx):
    inv_root = query_b.shape[-1] ** (-0.5)
    scores = masked_scores(query_b, keys_b, allowed)
    probs_f = jnp.exp(scores - log_total[..., None])
    probs_fb = probs_f.astype(jnp.bfloat16)
    grad_ctx_f = grad_ctx.astype(jnp.float32)
    grad_probs = jnp.einsum('qhd,khd->hqk', grad_ctx_f, vals_b.astype(jnp.float32))
    grad_vals = jnp.einsum('hqk,qhd->khd', probs_fb.astype(jnp.float32), grad_ctx_f)
    row_dot = lax.optimization_barrier(jnp.sum(grad_ctx_f * context, axis=-1)).T
    grad_scores = (probs_f * (grad_probs - row_dot[:, :, None]) * inv_root).astype(jnp.bfloat16)
    grad_query = jnp.einsum('hqk,khd->qhd', grad_scores.astype(jnp.float32), keys_b.astype(jnp.float32))
    grad_keys = jnp.einsum('hqk,qhd->khd', grad_scores.astype(jnp.float32), query_b.astype(jnp.float32))
    return (grad_query, grad_keys, grad_vals)

def block_pass(hidden_rows, cot_rows, seg_rows, params):
    gain_one, bias_one, w_qkv, b_qkv, w_dense, b_dense, gain_two, bias_two, w_up, b_up, w_down, b_down = params
    row_count = hidden_rows.shape[0]
    inputs_f = hidden_rows.astype(jnp.float32)
    cos_table, sin_table, allowed = rotary_angles(seg_rows)
    gain_one_f = gain_one.astype(jnp.float32)
    bias_one_f = bias_one.astype(jnp.float32)
    normed_one = layer_norm(inputs_f, gain_one_f, bias_one_f).astype(jnp.bfloat16)
    packed = jnp.dot(normed_one, w_qkv, preferred_element_type=jnp.float32) + b_qkv.astype(jnp.float32)
    query_pre = packed[:, :D].reshape(row_count, HEADS, HEAD)
    keys_pre = packed[:, D:2 * D].reshape(row_count, HEADS, HEAD)
    query_b = rotate(query_pre, cos_table, sin_table).astype(jnp.bfloat16)
    keys_b = rotate(keys_pre, cos_table, sin_table).astype(jnp.bfloat16)
    vals_b = packed[:, 2 * D:].reshape(row_count, HEADS, HEAD).astype(jnp.bfloat16)
    context, log_total = attention_forward(query_b, keys_b, vals_b, allowed)
    context_b = context.reshape(row_count, D).astype(jnp.bfloat16)
    attn_out = jnp.dot(context_b, w_dense, preferred_element_type=jnp.float32) + b_dense.astype(jnp.float32)
    gain_two_f = gain_two.astype(jnp.float32)
    bias_two_f = bias_two.astype(jnp.float32)
    normed_two = layer_norm(inputs_f, gain_two_f, bias_two_f).astype(jnp.bfloat16)
    pre_act = jnp.dot(normed_two, w_up, preferred_element_type=jnp.float32) + b_up.astype(jnp.float32)
    act_b = gelu_exact(pre_act).astype(jnp.bfloat16)
    mlp_out = jnp.dot(act_b, w_down, preferred_element_type=jnp.float32) + b_down.astype(jnp.float32)
    result = (inputs_f + attn_out + mlp_out).astype(jnp.bfloat16)
    cot_f = cot_rows.astype(jnp.float32)
    grad_w_down = jnp.dot(act_b.T, cot_rows, preferred_element_type=jnp.float32)
    grad_b_down = lax.optimization_barrier(jnp.sum(cot_f, axis=0))
    grad_act = jnp.dot(cot_rows, w_down.T, preferred_element_type=jnp.float32)
    grad_pre = jax.vjp(gelu_exact, pre_act)[1](grad_act)[0]
    grad_pre_b = grad_pre.astype(jnp.bfloat16)
    grad_w_up = jnp.dot(normed_two.T, grad_pre_b, preferred_element_type=jnp.float32)
    grad_b_up = lax.optimization_barrier(jnp.sum(grad_pre, axis=0))
    grad_normed_two = jnp.dot(grad_pre_b, w_up.T, preferred_element_type=jnp.float32)
    norm_back_two = jax.vjp(layer_norm, inputs_f, gain_two_f, bias_two_f)[1]
    grad_in_two, grad_gain_two, grad_bias_two = norm_back_two(grad_normed_two)
    grad_w_dense = jnp.dot(context_b.T, cot_rows, preferred_element_type=jnp.float32)
    grad_b_dense = lax.optimization_barrier(jnp.sum(cot_f, axis=0))
    grad_ctx = jnp.dot(cot_rows, w_dense.T, preferred_element_type=jnp.float32).astype(jnp.bfloat16).reshape(row_count, HEADS, HEAD)
    grad_query, grad_keys, grad_vals = attention_backward(query_b, keys_b, vals_b, allowed, log_total, context.reshape(row_count, HEADS, HEAD), grad_ctx)
    rotate_back = jax.vjp(partial(rotate, cos_table=cos_table, sin_table=sin_table), query_pre)[1]
    grad_query_pre = rotate_back(grad_query)[0]
    grad_keys_pre = rotate_back(grad_keys)[0]
    grad_packed = jnp.concatenate([grad_query_pre.reshape(row_count, D), grad_keys_pre.reshape(row_count, D), grad_vals.reshape(row_count, D)], axis=1)
    grad_packed_b = grad_packed.astype(jnp.bfloat16)
    grad_w_qkv = jnp.dot(normed_one.T, grad_packed_b, preferred_element_type=jnp.float32)
    grad_b_qkv = lax.optimization_barrier(jnp.sum(grad_packed, axis=0))
    grad_normed_one = jnp.dot(grad_packed_b, w_qkv.T, preferred_element_type=jnp.float32)
    norm_back_one = jax.vjp(layer_norm, inputs_f, gain_one_f, bias_one_f)[1]
    grad_in_one, grad_gain_one, grad_bias_one = norm_back_one(grad_normed_one)
    grad_rows = cot_f + grad_in_one + grad_in_two
    grads = (grad_gain_one, grad_bias_one, grad_w_qkv, grad_b_qkv, grad_w_dense, grad_b_dense, grad_gain_two, grad_bias_two, grad_w_up, grad_b_up, grad_w_down, grad_b_down)
    return (result, grad_rows, grads)

def reference(hidden_in, out_cotangent, segment_ids, ln1_gain, ln1_bias, qkv_weight, qkv_bias, dense_weight, dense_bias, ln2_gain, ln2_bias, fc1_weight, fc1_bias, fc2_weight, fc2_bias):
    params = (ln1_gain, ln1_bias, qkv_weight, qkv_bias, dense_weight, dense_bias, ln2_gain, ln2_bias, fc1_weight, fc1_bias, fc2_weight, fc2_bias)
    blocks = TOKENS // TOK_DEV
    hidden_blocks = hidden_in.reshape(blocks, TOK_DEV, D)
    cot_blocks = out_cotangent.reshape(blocks, TOK_DEV, D)
    seg_blocks = segment_ids.reshape(blocks, TOK_DEV)
    start_sums = tuple((jnp.zeros(one.shape, jnp.float32) for one in params))

    def one_block(running, inputs):
        result, grad_rows, grads = block_pass(inputs[0], inputs[1], inputs[2], params)
        return (tuple((a + b for a, b in zip(running, grads))), (result, grad_rows))
    sums, (results, grad_rows) = lax.scan(one_block, start_sums, (hidden_blocks, cot_blocks, seg_blocks))
    return (results.reshape(TOKENS, D), grad_rows.reshape(TOKENS, D), sums[0], sums[1], sums[2], sums[3], sums[4], sums[5], sums[6], sums[7], sums[8], sums[9], sums[10], sums[11])
```

```python
from functools import partial

import jax
import jax.numpy as jnp
from jax import lax
from jax.experimental import pallas as pl
from jax.experimental.pallas import tpu as pltpu
from jax.sharding import PartitionSpec as P

HEADS = 8
HEAD = 256
ROT = 64
NEG_FILL = -1e30
EPSILON = 1e-05
BF = jnp.bfloat16
F32 = jnp.float32
MESH = pl.DeviceIdType.MESH
ANY = pl.BlockSpec(memory_space=pl.ANY)
VMEM_LIMIT = 60 << 20


def dot(a, b, da, db):
    return lax.dot_general(a, b, (((da,), (db,)), ((), ())), preferred_element_type=F32)


def flat(v):
    return v.reshape((-1, v.shape[-1]))


class Place:
    def __init__(self, nbits):
        self.nbits = nbits
        self.s = lax.axis_index("shard")
        self.rep = lax.axis_index("replica")
        self.c = self.rep % 2
        self.r = self.rep // 2
        self.bits = [(self.r // 2 ** (nbits - 1 - b)) % 2 for b in range(nbits)]
        self.over_x = (1 - self.s, self.rep)
        self.over_core = (self.s, self.rep + 1 - 2 * self.c)
        self.diagonal = (1 - self.s, self.rep + 1 - 2 * self.c)

    def over_bit(self, b):
        return (self.s, self.rep + (1 - 2 * self.bits[b]) * 2 ** (self.nbits - b))

    def peers(self):
        return [self.over_x, self.over_core, self.diagonal] + [
            self.over_bit(b) for b in range(self.nbits)
        ]

    def barrier(self):
        sem = pltpu.get_barrier_semaphore()
        for peer in self.peers():
            pl.semaphore_signal(sem, inc=1, device_id=peer, device_id_type=MESH)
        pl.semaphore_wait(sem, 3 + self.nbits)


class Mover:
    def __init__(self, send, recv, local):
        self.send, self.recv, self.local_sems = send, recv, local
        self.n = self.m = 0
        self.sent = []

    def remote(self, src, dst, peer):
        one = pltpu.make_async_remote_copy(
            src_ref=src,
            dst_ref=dst,
            send_sem=self.send.at[self.n],
            recv_sem=self.recv.at[self.n],
            device_id=peer,
            device_id_type=MESH,
        )
        self.n += 1
        one.start()
        self.sent.append(one)
        return one

    def local(self, src, dst):
        one = pltpu.make_async_copy(src, dst, self.local_sems.at[self.m])
        self.m += 1
        one.start()
        return one

    def finish(self):
        for one in self.sent:
            one.wait_send()


def arrived(copies):
    for one in copies:
        one.wait_recv()


def pipe(body, grid, ins, outs):
    pltpu.emit_pipeline(
        body,
        grid=grid,
        in_specs=[pl.BlockSpec(b, m) for _, b, m in ins],
        out_specs=[pl.BlockSpec(b, m) for _, b, m in outs],
    )(*[r for r, _, _ in ins], *[r for r, _, _ in outs])


def ds(start, size, step=None):
    return pl.ds(pl.multiple_of(start, step or size), size)


def gather_kernel(
    nbits,
    hid, cot, tab, small, wqkv, wdense, wfc1, wfc2,
    xall, call, tall, wq, wf1, n1, n2, st, gctx, gact, vec,
    own_x, own_c, own_t, own_q, own_f, sm_own, sm_got, sm, send, recv, lsem,
):
    me = Place(nbits)
    s, c, r = me.s, me.c, me.r
    rows, width = hid.shape
    half = wqkv.shape[0]
    quarter = width // 4
    ffq = wfc1.shape[1] // 4
    groups = 2**nbits
    own_rows = half // groups
    mine = tuple(me.bits)
    mv = Mover(send, recv, lsem)

    pull = [
        mv.local(hid, own_x),
        mv.local(cot, own_c),
        mv.local(tab, own_t),
        mv.local(small, sm_own),
        mv.local(wfc1.at[:, ds((2 * s + c) * ffq, ffq)], own_f),
    ] + [
        mv.local(
            wqkv.at[:, ds(g * width + (2 * s + c) * quarter, quarter)],
            own_q.at[:, pl.ds(g * quarter, quarter)],
        )
        for g in range(3)
    ]
    me.barrier()

    away = 2 * (1 - s) + c
    x_small = mv.remote(small, sm_got, me.over_x)
    chunk = ds(r * own_rows, own_rows)
    x_f1 = [mv.remote(wfc1.at[chunk, ds(away * ffq, ffq)], wf1.at[(s,) + mine], me.over_x)]
    x_q = [
        mv.remote(
            wqkv.at[chunk, ds(g * width + away * quarter, quarter)],
            wq.at[(s,) + mine + (slice(None), pl.ds(g * quarter, quarter))],
            me.over_x,
        )
        for g in range(3)
    ]
    c_cot = mv.remote(cot, call.at[1], me.over_core)
    c_hid = mv.remote(hid, xall.at[1], me.over_core)
    c_tab = mv.remote(tab, tall.at[1], me.over_core)
    x_tab = mv.remote(tab, tall.at[2], me.over_x)
    x_cot = mv.remote(cot, call.at[2], me.over_x)

    for one in pull:
        one.wait()
    push = [
        mv.local(own_c, call.at[0]),
        mv.local(own_x, xall.at[0]),
        mv.local(own_t, tall.at[0]),
    ]
    for k in range(groups):
        at = (s,) + tuple((k // 2 ** (nbits - 1 - b)) % 2 for b in range(nbits))
        push.append(mv.local(own_f.at[pl.ds(k * own_rows, own_rows)], wf1.at[at]))
        push.append(mv.local(own_q.at[pl.ds(k * own_rows, own_rows)], wq.at[at]))

    def spread(w, b):
        at = tuple(slice(None) if k < b else me.bits[k] for k in range(nbits))
        return [mv.remote(w.at[(1 - s,) + at], w.at[(1 - s,) + at], me.over_bit(b))]

    for one in push:
        one.wait()
    arrived([c_cot])

    def from_cot(blocks):
        cots = call.at[blocks]
        count = cots.shape[0]
        tile = min(512, ffq)

        def body(a, b, o):
            o[0] = dot(a[0], b[...], 1, 1)

        pipe(
            body,
            (ffq // tile, count),
            [
                (cots, (1, rows, width), lambda j, i: (i, 0, 0)),
                (wfc2.at[ds(c * ffq, ffq)], (tile, width), lambda j, i: (j, 0)),
            ],
            [(gact.at[blocks], (1, rows, tile), lambda j, i: (i, 0, j))],
        )

        def body_b(a, b, o):
            o[0] = dot(a[0], b[...], 1, 1).astype(BF)

        pipe(
            body_b,
            (count,),
            [
                (cots, (1, rows, width), lambda i: (i, 0, 0)),
                (wdense.at[ds(c * quarter, quarter)], (quarter, width), lambda i: (0, 0)),
            ],
            [(gctx.at[blocks], (1, rows, quarter), lambda i: (i, 0, 0))],
        )

    arrived(x_f1)
    f1 = spread(wf1, 0)
    arrived(x_q)
    q = spread(wq, 0)

    from_cot(pl.ds(0, 2))

    for b in range(1, nbits):
        arrived(f1)
        f1 = spread(wf1, b)
        if b == 1:
            arrived([x_small, c_hid, c_tab])
            lo = 0
            for n in (half, half, half, half, 3 * half, ffq * 2, half, half):
                sm[:, ds(2 * lo + s * n, n, 128)] = sm_own[:, pl.ds(lo, n)]
                sm[:, ds(2 * lo + (1 - s) * n, n, 128)] = sm_got[:, pl.ds(lo, n)]
                lo += n
            norm_blocks(rows, width, xall.at[pl.ds(0, 2)], n1.at[pl.ds(0, 2)], n2.at[pl.ds(0, 2)], st.at[pl.ds(0, 2)], sm)
        arrived(q)
        q = spread(wq, b)

    arrived([x_cot])
    d_cot = mv.remote(call.at[2], call.at[3], me.over_core)
    x_hid = mv.remote(hid, xall.at[2], me.over_x)
    arrived([d_cot])
    from_cot(pl.ds(2, 2))
    arrived([x_tab])
    d_tab = mv.remote(tall.at[2], tall.at[3], me.over_core)
    keep = mv.local(sm, vec)
    arrived(f1)
    arrived(q)
    arrived([x_hid])
    d_hid = mv.remote(xall.at[2], xall.at[3], me.over_core)
    norm_blocks(rows, width, xall.at[pl.ds(2, 1)], n1.at[pl.ds(2, 1)], n2.at[pl.ds(2, 1)], st.at[pl.ds(2, 1)], sm)
    arrived([d_hid])
    norm_blocks(rows, width, xall.at[pl.ds(3, 1)], n1.at[pl.ds(3, 1)], n2.at[pl.ds(3, 1)], st.at[pl.ds(3, 1)], sm)
    arrived([d_tab])
    keep.wait()
    mv.finish()


def norm_blocks(rows, width, x, n1, n2, st, sm):
    tile = rows // 2

    def body(x, o1, o2, ost):
        xf = x[0].astype(F32)
        mean = jnp.mean(xf, axis=1, keepdims=True)
        center = xf - mean
        spread = jnp.mean(center * center, axis=1, keepdims=True)
        rstd = lax.rsqrt(spread + EPSILON)
        n = center * rstd
        o1[0] = (n * sm[:, pl.ds(0, width)] + sm[:, pl.ds(width, width)]).astype(BF)
        o2[0] = (n * sm[:, pl.ds(2 * width, width)] + sm[:, pl.ds(3 * width, width)]).astype(BF)
        lane = lax.broadcasted_iota(jnp.int32, (tile, 128), 1)
        ost[0] = jnp.where(lane == 0, mean, rstd)

    at = lambda i, j: (i, j, 0)
    pipe(
        body,
        (x.shape[0], 2),
        [(x, (1, tile, width), at)],
        [(n1, (1, tile, width), at), (n2, (1, tile, width), at), (st, (1, tile, 128), at)],
    )


def gather(nbits, hid, cot, tab, small, wqkv, wdense, wfc1, wfc2):
    rows, width = hid.shape
    half = wqkv.shape[0]
    quarter, ffq = width // 4, wfc1.shape[1] // 4
    groups = 2**nbits
    own_rows = half // groups
    length = small.shape[1]
    sds = jax.ShapeDtypeStruct
    dims = (2,) * (1 + nbits) + (own_rows,)
    return pl.pallas_call(
        partial(gather_kernel, nbits),
        in_specs=[ANY] * 8,
        out_specs=[ANY] * 11,
        out_shape=[
            sds((4, rows, width), BF),
            sds((4, rows, width), BF),
            sds((4, rows, 128), F32),
            sds(dims + (3 * quarter,), BF),
            sds(dims + (ffq,), BF),
            sds((4, rows, width), BF),
            sds((4, rows, width), BF),
            sds((4, rows, 128), F32),
            sds((4, rows, quarter), BF),
            sds((4, rows, ffq), F32),
            sds((1, 2 * length), F32),
        ],
        scratch_shapes=[
            pltpu.VMEM((rows, width), BF),
            pltpu.VMEM((rows, width), BF),
            pltpu.VMEM((rows, 128), F32),
            pltpu.VMEM((half, 3 * quarter), BF),
            pltpu.VMEM((half, ffq), BF),
            pltpu.VMEM((1, length), F32),
            pltpu.VMEM((1, length), F32),
            pltpu.VMEM((1, 2 * length), F32),
            pltpu.SemaphoreType.DMA((16 + 2 * nbits,)),
            pltpu.SemaphoreType.DMA((16 + 2 * nbits,)),
            pltpu.SemaphoreType.DMA((12 + 2 * groups,)),
        ],
        compiler_params=pltpu.CompilerParams(
            collective_id=0, has_side_effects=True, vmem_limit_bytes=VMEM_LIMIT
        ),
        name="gather",
    )(hid, cot, tab, small, wqkv, wdense, wfc1, wfc2)


class Reduce:
    def __init__(self, me, mv, g, order, pre, got, sums):
        self.me, self.mv, self.g, self.order, self.pre = me, mv, g, order, pre
        self.got, self.sums = got, sums
        self.step = 0
        self.flying = None

    def view(self, level, last):
        ref = self.g if level == 0 else self.got[level - 1]
        gone = self.order[:level]
        at = [slice(None)] * self.pre
        for b in range(self.me.nbits):
            if b in gone:
                continue
            if b in self.order[: self.step]:
                at.append(self.me.bits[b])
            elif self.step < len(self.order) and b == self.order[self.step]:
                at.append(last)
            else:
                at.append(slice(None))
        return ref.at[tuple(at)]

    def go(self):
        if self.flying is not None:
            self.flying.wait_recv()
        b = self.order[self.step]
        other = 1 - self.me.bits[b]
        if self.step == 0:
            src = self.view(0, other)
        else:
            src = self.sums[self.step - 1]
            add_up([self.view(k, other) for k in range(self.step + 1)], src)
        self.flying = self.mv.remote(src, self.got[self.step], self.me.over_bit(b))
        self.step += 1

    def end(self, out):
        self.flying.wait_recv()
        add_up([self.view(k, None) for k in range(self.step + 1)], out)


def add_up(sources, out):
    shape = sources[0].shape
    lead = len(shape) - 2
    size = shape[-2] * shape[-1]
    whole = [1] * lead
    grid = []
    for d in reversed(range(lead)):
        if size * shape[d] <= (1 << 18) and not grid:
            whole[d] = shape[d]
            size *= shape[d]
        else:
            grid.insert(0, d)
    if not grid:
        grid = [0] if lead else []
    block = tuple(whole) + shape[-2:]
    split = 1
    rows = shape[-2]
    if not grid:
        split = 2 if rows % 32 == 0 else 1
        block = (rows // split, shape[-1])

        def index(i):
            return (i, 0)

        steps = (split,)
    else:
        steps = tuple(shape[d] // whole[d] for d in grid)

        def index(*g):
            at = [0] * len(shape)
            for d, i in zip(grid, g):
                at[d] = i
            return tuple(at)

    out_block = block
    folded = len(out.shape) != len(shape)
    if folded:
        out_block = block[:-2] + out.shape[-3:]

    def out_index(*g):
        at = index(*g)
        return at[:-2] + (0, 0, 0) if folded else at

    def body(*refs):
        total = refs[0][...].astype(F32)
        for one in refs[1:-1]:
            total = total + one[...].astype(F32)
        refs[-1][...] = total.astype(refs[-1].dtype).reshape(out_block)

    pipe(
        body,
        steps,
        [(v, block, index) for v in sources],
        [(out, out_block, out_index)],
    )


def attention_body(packed, gctx, tab, ctx_out, grad_out, sums):
    rows, width = gctx.shape[1:]
    t = tab[0]
    lane = lax.broadcasted_iota(jnp.int32, (rows, 128), 1)
    quart = ROT // 2
    cos = jnp.where(lane < quart, t, jnp.where(lane < ROT, pltpu.roll(t, quart, 1), 1.0))
    sin = jnp.where(lane < quart, -pltpu.roll(t, 128 - quart, 1), jnp.where(lane < ROT, t, 0.0))

    def rotate(v, sign):
        low = v[:, :128]
        swapped = jnp.where(
            lane < quart, pltpu.roll(low, 128 - quart, 1), pltpu.roll(low, quart, 1)
        )
        return jnp.concatenate([low * cos + swapped * (sign * sin), v[:, 128:]], axis=1)

    row = lax.broadcasted_iota(jnp.int32, (rows, rows), 0)
    col = lax.broadcasted_iota(jnp.int32, (rows, rows), 1)
    allowed = (t[:, ROT : ROT + 1] == t.T[ROT : ROT + 1, :]) & (col <= row)
    inv_root = HEAD ** (-0.5)
    for h in range(width // HEAD):
        cq = pl.ds(h * HEAD, HEAD)
        ck = pl.ds(width + h * HEAD, HEAD)
        cv = pl.ds(2 * width + h * HEAD, HEAD)
        q = rotate(packed[0, :, cq], 1.0).astype(BF)
        k = rotate(packed[0, :, ck], 1.0).astype(BF)
        v = packed[0, :, cv].astype(BF)
        g = gctx[0, :, cq]
        scores = jnp.where(allowed, dot(q, k, 1, 1) * inv_root, NEG_FILL)
        peak = jnp.max(scores, axis=1, keepdims=True)
        e = jnp.exp(scores - peak)
        total = jnp.sum(e, axis=1, keepdims=True)
        probs = e * (1.0 / total)
        probs_b = probs.astype(BF)
        context = dot(probs_b, v, 1, 0)
        ctx_out[0, :, cq] = context.astype(BF)
        row_dot = jnp.sum(g.astype(F32) * context, axis=1, keepdims=True)
        grad_probs = dot(g, v, 1, 1)
        grad_scores = (probs * (grad_probs - row_dot) * inv_root).astype(BF)
        gv = dot(probs_b, g, 0, 0)
        gq = rotate(dot(grad_scores, k, 1, 0), -1.0)
        gk = rotate(dot(grad_scores, q, 0, 0), -1.0)
        for cols, grad in ((cq, gq), (ck, gk), (cv, gv)):
            grad_out[0, :, cols] = grad.astype(BF)
            sums[0, :, cols] = jnp.broadcast_to(
                jnp.sum(grad, axis=0, keepdims=True), (8, HEAD)
            )


def gelu_and_slope(a):
    half_erf = 0.5 * lax.erf(a * 0.7071067811865476)
    cdf = 0.5 + half_erf
    slope = cdf + a * (jnp.exp(-0.5 * a * a) * 0.3989422804014327)
    return a * cdf, slope


def layer_kernel(nbits, nd, *refs):
    (
        xall, call, tall, wq, wf1, n1, n2, st, gctx, gact, vec, wdense, wfc2,
        act, gpre, fsum, packed, ctx, gpk, qsum,
        f2, f2s, g1, d, d_s, gq,
        outp, outr, outs, outx, up, ur, us, ux, usum,
    ) = refs[:35]
    rs = refs[35 : 35 + nd]
    send, recv, lsem = refs[35 + nd :]
    me = Place(nbits)
    s, c = me.s, me.c
    blocks, rows, width = xall.shape
    quarter = gctx.shape[2]
    ffq = gact.shape[2]
    lead = (0,) * (2 + nbits)
    wdims = wq.shape[:-1]
    own_rows = wdims[-1]
    mv = Mover(send, recv, lsem)
    me.barrier()
    bias_q_at = 4 * width
    bias_f_at = 7 * width

    per = nbits * 2 - 1

    def reduction(k, g, order, pre):
        mine = rs[k * per : (k + 1) * per]
        return Reduce(me, mv, g, order, pre, mine[:nbits], mine[nbits:])

    usual = tuple(reversed(range(nbits)))
    swapped = (usual[1], usual[0]) + usual[2:] if nbits > 1 else usual

    tile = min(512, ffq)

    def fc1_body(a, w, g, b, o_act, o_pre, o_sum):
        pre = dot(a[0], flat(w[...]), 1, 0) + b[...]
        value, slope = gelu_and_slope(pre)
        o_act[0] = value.astype(BF)
        grad = g[0] * slope
        o_pre[0] = grad.astype(BF)
        o_sum[0] = jnp.broadcast_to(jnp.sum(grad, axis=0, keepdims=True), (8, tile))

    pipe(
        fc1_body,
        (ffq // tile, blocks),
        [
            (n2, (1, rows, width), lambda j, i: (i, 0, 0)),
            (wf1, wdims + (tile,), lambda j, i: lead + (j,)),
            (gact, (1, rows, tile), lambda j, i: (i, 0, j)),
            (vec.at[:, ds(bias_f_at + (2 * s + c) * ffq, ffq, 128)], (1, tile), lambda j, i: (0, j)),
        ],
        [
            (act, (1, rows, tile), lambda j, i: (i, 0, j)),
            (gpre, (1, rows, tile), lambda j, i: (i, 0, j)),
            (fsum, (1, 8, tile), lambda j, i: (i, 0, j)),
        ],
    )

    def row_grad(lhs, keep, away, cols_tile):
        per_owner = keep.shape[-2]
        dims = keep.shape[:-2]
        lw = lhs.shape[2]

        def body(a, b, o_keep, o_away):
            full = dot(flat(a[...]), flat(b[...]), 0, 0).astype(BF)
            full = full.reshape((lw // (2 * per_owner), 2, per_owner, full.shape[-1]))
            zero, one = full[:, 0], full[:, 1]
            o_keep[...] = jnp.where(c == 0, zero, one).reshape(o_keep.shape)
            o_away[...] = jnp.where(c == 0, one, zero).reshape(o_away.shape)

        block = dims + (per_owner, cols_tile)
        at = lambda j: (0,) * (len(dims) + 1) + (j,)
        pipe(
            body,
            (width // cols_tile,),
            [
                (lhs, (blocks, rows, lw), lambda j: (0, 0, 0)),
                (call, (blocks, rows, cols_tile), lambda j: (0, 0, j)),
            ],
            [(keep, block, at), (away, block, at)],
        )

    def column_grad(lhs, rhs, out):
        cols = rhs.shape[2]
        block = (1, 1) + out.shape[2:]
        high = width // 4

        def body(a, b, o):
            full = dot(flat(a[...]), flat(b[...]), 0, 0).astype(BF)
            o[...] = full.reshape(block)

        pipe(
            body,
            (2, 2),
            [
                (lhs, (blocks, rows, high), lambda i, j: (0, 0, i * 2 + j)),
                (rhs, (blocks, rows, cols), lambda i, j: (0, 0, 0)),
            ],
            [(out, block, lambda i, j: (i, j) + (0,) * (len(block) - 2))],
        )

    row_grad(act, f2.at[c], f2s, 512)
    f2_swap = mv.remote(f2s, f2.at[c], me.over_core)
    red_f2 = reduction(0, f2, usual, 0)
    column_grad(n2, gpre, g1)
    red_f1 = reduction(1, g1, swapped, 1)
    red_f1.go()
    f2_swap.wait_recv()
    red_f2.go()

    def qkv_body(a, w, b, o):
        o[0] = dot(a[0], flat(w[...]), 1, 0) + b[...]

    pipe(
        qkv_body,
        (3, blocks),
        [
            (n1, (1, rows, width), lambda j, i: (i, 0, 0)),
            (wq, wdims + (quarter,), lambda j, i: lead + (j,)),
            (vec.at[:, ds(bias_q_at, 3 * width, 128)], (1, quarter), lambda j, i: (0, j * 4 + 2 * s + c)),
        ],
        [(packed, (1, rows, quarter), lambda j, i: (i, 0, j))],
    )
    whole = lambda i: (i, 0, 0)
    pipe(
        attention_body,
        (blocks,),
        [
            (packed, (1, rows, 3 * quarter), whole),
            (gctx, (1, rows, quarter), whole),
            (tall, (1, rows, 128), whole),
        ],
        [
            (ctx, (1, rows, quarter), whole),
            (gpk, (1, rows, 3 * quarter), whole),
            (qsum, (1, 8, 3 * quarter), whole),
        ],
    )
    row_grad(ctx, d.at[c], d_s, 512)
    d_swap = mv.remote(d_s, d.at[c], me.over_core)
    red_d = reduction(2, d, usual, 0)
    red_f1.go()
    red_f2.go()
    d_swap.wait_recv()
    red_d.go()
    column_grad(n1, gpk, gq)
    red_q = reduction(3, gq, usual, 1)
    red_q.go()

    otile = 512

    def out_body(a, b, wa, wb, o):
        o[0] = (dot(a[0], wa[...], 1, 0) + dot(b[0], wb[...], 1, 0)).astype(BF)

    def out_part(at):
        pipe(
            out_body,
            (width // otile, 2),
            [
                (ctx.at[at], (1, rows, quarter), lambda j, i: (i, 0, 0)),
                (act.at[at], (1, rows, ffq), lambda j, i: (i, 0, 0)),
                (wdense.at[ds(c * quarter, quarter)], (quarter, otile), lambda j, i: (0, j)),
                (wfc2.at[ds(c * ffq, ffq)], (ffq, otile), lambda j, i: (0, j)),
            ],
            [(outp.at[at], (1, rows, otile), lambda j, i: (i, 0, j))],
        )

    def in_body(a, b, wa, wb, x, stat, g1v, g2v, o, osum):
        one = dot(a[0], flat(wa[...]), 1, 1)
        two = dot(b[0], flat(wb[...]), 1, 1)
        mean, rstd = stat[0, :, 0:1], stat[0, :, 1:2]
        n = (x[0].astype(F32) - mean) * rstd
        o[0] = (one * g1v[...] + two * g2v[...]).astype(BF)
        osum[0, 0:1, :] = jnp.sum(one * n, axis=0, keepdims=True)
        osum[0, 1:2, :] = jnp.sum(one, axis=0, keepdims=True)
        osum[0, 2:3, :] = jnp.sum(two * n, axis=0, keepdims=True)
        osum[0, 3:4, :] = jnp.sum(two, axis=0, keepdims=True)

    wblock = (1, 1) + wdims[2:]
    wide = width // 4

    def in_part(at):
        wat = lambda i, j, t: (i, j) + (0,) * (nbits + 1)
        col = lambda i, j, t: (t, 0, i * 2 + j)
        tok = lambda i, j, t: (t, 0, 0)
        row = lambda i, j, t: (0, i * 2 + j)
        pipe(
            in_body,
            (2, 2, 2),
            [
                (gpk.at[at], (1, rows, 3 * quarter), tok),
                (gpre.at[at], (1, rows, ffq), tok),
                (wq, wblock + (3 * quarter,), wat),
                (wf1, wblock + (ffq,), wat),
                (xall.at[at], (1, rows, wide), col),
                (st.at[at], (1, rows, 128), tok),
                (vec.at[:, pl.ds(0, width)], (1, wide), row),
                (vec.at[:, pl.ds(2 * width, width)], (1, wide), row),
            ],
            [
                (up.at[at], (1, rows, wide), col),
                (usum.at[at], (1, 8, wide), col),
            ],
        )

    far, near = pl.ds(2, 2), pl.ds(0, 2)
    out_part(far)
    oc3 = mv.remote(outp.at[3], outr.at[1], me.over_core)
    out_part(near)
    oc1 = mv.remote(outp.at[1], outr.at[0], me.over_core)
    oc3.wait_recv()
    add_up([outp.at[2], outr.at[1]], outs)
    ox = mv.remote(outs, outx, me.over_x)
    in_part(far)
    uc3 = mv.remote(up.at[3], ur.at[1], me.over_core)
    red_d.go()
    red_q.go()
    red_f2.go()
    red_f1.go()
    uc3.wait_recv()
    add_up([up.at[2], ur.at[1]], us)
    ux_ = mv.remote(us, ux, me.over_x)
    in_part(near)
    uc1 = mv.remote(up.at[1], ur.at[0], me.over_core)
    for _ in range(nbits):
        for one in (red_f2, red_f1, red_d, red_q):
            if one.step < nbits:
                one.go()
    o_f2, o_d, e_f1, e_q, r_f1, r_q = rs[4 * per :]
    red_f2.end(o_f2)
    last = []

    def hand_over(red, e, got):
        red.end(e)
        last.append(mv.remote(e.at[s, 1 - c], got.at[0], me.over_core))
        last.append(mv.remote(e.at[1 - s, c], got.at[1], me.over_x))
        last.append(mv.remote(e.at[1 - s, 1 - c], got.at[2], me.diagonal))

    hand_over(red_f1, e_f1, r_f1)
    red_d.end(o_d)
    hand_over(red_q, e_q, r_q)
    arrived(last)
    arrived([oc1, ox, uc1, ux_])
    mv.finish()


def layer(nbits, xall, call, tall, wq, wf1, n1, n2, st, gctx, gact, vec, wdense, wfc2):
    blocks, rows, width = xall.shape
    quarter, ffq = gctx.shape[2], gact.shape[2]
    own_rows = wq.shape[-2]
    sds = jax.ShapeDtypeStruct
    bits = (2,) * nbits
    usual = tuple(reversed(range(nbits)))
    per_ff = ffq // 2 ** nbits
    half_own = own_rows // 2
    outs = [
        sds((blocks, rows, ffq), BF),
        sds((blocks, rows, ffq), BF),
        sds((blocks, 8, ffq), F32),
        sds((blocks, rows, 3 * quarter), F32),
        sds((blocks, rows, quarter), BF),
        sds((blocks, rows, 3 * quarter), BF),
        sds((blocks, 8, 3 * quarter), F32),
        sds(bits + (per_ff, width), BF),
        sds(bits[1:] + (per_ff, width), BF),
        sds((2,) + bits + (own_rows, ffq), BF),
        sds(bits + (half_own, width), BF),
        sds(bits[1:] + (half_own, width), BF),
        sds((2,) + bits + (own_rows, 3 * quarter), BF),
        sds((blocks, rows, width), BF),
        sds((2, rows, width), BF),
        sds((rows, width), BF),
        sds((rows, width), BF),
        sds((blocks, rows, width), BF),
        sds((2, rows, width), BF),
        sds((rows, width), BF),
        sds((rows, width), BF),
        sds((blocks, 8, width), F32),
    ]
    extra = []
    for pre, tail in (
        ((), (per_ff, width)),
        ((2,), (own_rows, ffq)),
        ((), (half_own, width)),
        ((2,), (own_rows, 3 * quarter)),
    ):
        extra += [sds(pre + (2,) * (nbits - 1 - t) + tail, BF) for t in range(nbits)]
        extra += [sds(pre + (2,) * (nbits - 1 - t) + tail, BF) for t in range(1, nbits)]
    extra += [
        sds((per_ff, width), F32),
        sds((half_own, width), F32),
        sds((2, 2, half_own, ffq), BF),
        sds((2, 2, half_own, 3 * quarter), BF),
        sds((3, half_own, ffq), BF),
        sds((3, half_own, 3 * quarter), BF),
    ]
    copies = 4 * nbits + 14
    got = pl.pallas_call(
        partial(layer_kernel, nbits, len(extra)),
        in_specs=[ANY] * 13,
        out_specs=[ANY] * (len(outs) + len(extra)),
        out_shape=outs + extra,
        scratch_shapes=[
            pltpu.SemaphoreType.DMA((copies,)),
            pltpu.SemaphoreType.DMA((copies,)),
            pltpu.SemaphoreType.DMA((4,)),
        ],
        compiler_params=pltpu.CompilerParams(
            collective_id=1, has_side_effects=True, vmem_limit_bytes=VMEM_LIMIT
        ),
        name="layer",
    )(xall, call, tall, wq, wf1, n1, n2, st, gctx, gact, vec, wdense, wfc2)
    outs, extra = got[: len(outs)], got[len(outs) :]
    return outs, extra[-6:]


def small_sum_kernel(nbits, own, out, acc, got, send, recv):
    me = Place(nbits)
    me.barrier()
    peers = [me.over_x, me.over_core] + [me.over_bit(b) for b in range(nbits)]
    copies = []
    for k, peer in enumerate(peers):
        one = pltpu.make_async_remote_copy(
            src_ref=own if k == 0 else acc.at[k - 1],
            dst_ref=got.at[k],
            send_sem=send.at[k],
            recv_sem=recv.at[k],
            device_id=peer,
            device_id_type=MESH,
        )
        one.start()
        copies.append(one)
        one.wait_recv()
        so_far = own[...] if k == 0 else acc[k - 1]
        acc[k] = so_far + got[k]
    out[...] = acc[len(peers) - 1]
    for one in copies:
        one.wait_send()


def small_sum(nbits, v):
    stages = 2 + nbits
    spec = pl.BlockSpec(memory_space=pltpu.VMEM)
    return pl.pallas_call(
        partial(small_sum_kernel, nbits),
        in_specs=[spec],
        out_specs=spec,
        out_shape=jax.ShapeDtypeStruct(v.shape, F32),
        scratch_shapes=[
            pltpu.VMEM((stages,) + v.shape, F32),
            pltpu.VMEM((stages,) + v.shape, F32),
            pltpu.SemaphoreType.DMA((stages,)),
            pltpu.SemaphoreType.DMA((stages,)),
        ],
        compiler_params=pltpu.CompilerParams(collective_id=2, has_side_effects=True),
        name="small_sum",
    )(v)


def rotary_table(seg):
    rows = seg.shape[0]
    index = jnp.arange(rows, dtype=jnp.int32)
    same = seg[:, None] == seg[None, :]
    first = jnp.min(jnp.where(same, index[None, :], rows), axis=1)
    offset = (index - first).astype(F32)
    frequency = jnp.exp(-jnp.log(10000.0) * jnp.arange(0, ROT, 2).astype(F32) / ROT)
    angles = offset[:, None] * frequency[None, :]
    ids = jnp.broadcast_to(seg.astype(F32)[:, None], (rows, 128 - ROT))
    return jnp.concatenate([jnp.cos(angles), jnp.sin(angles), ids], axis=1)


def local(
    nbits,
    hidden_in,
    out_cotangent,
    segment_ids,
    ln1_gain,
    ln1_bias,
    qkv_weight,
    qkv_bias,
    dense_weight,
    dense_bias,
    ln2_gain,
    ln2_bias,
    fc1_weight,
    fc1_bias,
    fc2_weight,
    fc2_bias,
):
    s = lax.axis_index("shard")
    rep = lax.axis_index("replica")
    c = rep % 2
    groups = 2**nbits
    owners = 4 * groups
    rows, width = hidden_in.shape
    quarter = width // 4
    ff = fc1_weight.shape[1]
    ffq = ff // 4

    small = jnp.concatenate(
        [ln1_gain, ln1_bias, ln2_gain, ln2_bias, qkv_bias, fc1_bias, dense_bias, fc2_bias]
    ).astype(F32)[None]
    tab = rotary_table(segment_ids)
    xall, call, tall, wq, wf1, n1, n2, st, gctx, gact, vec = gather(
        nbits, hidden_in, out_cotangent, tab, small, qkv_weight, dense_weight, fc1_weight, fc2_weight
    )
    outs, (o_fc2, o_dense, e_f1, e_q, r_f1, r_q) = layer(
        nbits, xall, call, tall, wq, wf1, n1, n2, st, gctx, gact, vec, dense_weight, fc2_weight
    )
    fsum, qsum, outp, outr, outx = outs[2], outs[6], outs[13], outs[14], outs[16]
    up, ur, ux, usum = outs[17], outs[18], outs[20], outs[21]

    xf = hidden_in.astype(F32)
    cot_f = out_cotangent.astype(F32)
    bias = vec[:, -2 * width : -width] + vec[:, -width:]
    result = (
        xf + (outp[0].astype(F32) + outr[0].astype(F32) + outx.astype(F32) + bias)
    ).astype(BF)
    u = up[0].astype(F32) + ur[0].astype(F32) + ux.astype(F32)
    center = xf - jnp.mean(xf, axis=-1, keepdims=True)
    rstd = lax.rsqrt(jnp.mean(center * center, axis=-1, keepdims=True) + EPSILON)
    n = center * rstd
    grad_rows = cot_f + rstd * (
        u - jnp.mean(u, axis=-1, keepdims=True) - n * jnp.mean(u * n, axis=-1, keepdims=True)
    )

    def columns(e, got):
        own = lax.dynamic_slice(e, (s, c, 0, 0), (1, 1) + e.shape[2:])[0, 0]
        both = jnp.stack([jnp.stack([own, got[0]]), jnp.stack([got[1], got[2]])])
        both = jnp.where(c == 0, both, both[:, ::-1])
        return jnp.where(s == 0, both, both[::-1]).astype(F32)

    own_rows = width // owners
    o_fc1 = columns(e_f1, r_f1).transpose(2, 0, 1, 3).reshape(own_rows, ff)
    o_qkv = (
        columns(e_q, r_q)
        .reshape(2, 2, own_rows, 3, quarter)
        .transpose(2, 3, 0, 1, 4)
        .reshape(own_rows, 3 * width)
    )

    usums = jnp.sum(usum[:, :4], axis=0)
    gb_qkv = lax.dynamic_update_slice(
        jnp.zeros((3, width), F32),
        jnp.sum(qsum[:, 0], axis=0).reshape(3, quarter),
        (0, (2 * s + c) * quarter),
    )
    gb_fc1 = lax.dynamic_update_slice(
        jnp.zeros((ff,), F32), jnp.sum(fsum[:, 0], axis=0), ((2 * s + c) * ffq,)
    )
    pack = jnp.concatenate(
        [
            v.reshape(owners, -1)
            for v in (usums[0], usums[1], usums[2], usums[3], jnp.sum(cot_f, axis=0), gb_qkv, gb_fc1)
        ],
        axis=1,
    )
    total = small_sum(nbits, pack)
    mine = lax.dynamic_index_in_dim(total, s * 2 * groups + rep, 0, keepdims=False)
    o_g1, o_b1, o_g2, o_b2, o_down = (
        mine[i * own_rows : (i + 1) * own_rows] for i in range(5)
    )
    o_bqkv = mine[5 * own_rows : 8 * own_rows]
    o_bfc1 = mine[8 * own_rows :]
    return (
        result,
        grad_rows,
        o_g1,
        o_b1,
        o_qkv,
        o_bqkv,
        o_dense,
        o_down,
        o_g2,
        o_b2,
        o_fc1,
        o_bfc1,
        o_fc2,
        o_down,
    )


def solution(mesh):
    both = ("shard", "replica")
    nbits = (mesh.shape["replica"] // 2).bit_length() - 1
    wide, token, vector, matrix = P(both, None), P(both), P("shard"), P("shard", None)
    return jax.shard_map(
        partial(local, nbits),
        mesh=mesh,
        in_specs=(wide, wide, token, vector, vector, matrix, vector, matrix, vector)
        + (vector, vector, matrix, vector, matrix, vector),
        out_specs=(wide, wide, token, token, wide, token, wide, token)
        + (token, token, wide, token, wide, token),
        check_vma=False,
    )
```

```python
from functools import partial

import jax
import jax.numpy as jnp
from jax import lax
from jax.experimental import pallas as pl
from jax.experimental.pallas import tpu as pltpu
from jax.sharding import PartitionSpec as P

HEADS = 8
HEAD = 256
ROT = 64
NEG_FILL = -1e30
EPSILON = 1e-05
BF = jnp.bfloat16
F32 = jnp.float32
MESH = pl.DeviceIdType.MESH
ANY = pl.BlockSpec(memory_space=pl.ANY)
VMEM_LIMIT = 62 << 20


def dot(a, b, da, db):
    return lax.dot_general(a, b, (((da,), (db,)), ((), ())), preferred_element_type=F32)


def flat(v):
    return v.reshape((-1, v.shape[-1]))


class Place:
    def __init__(self, nbits):
        self.nbits = nbits
        self.s = lax.axis_index("shard")
        self.rep = lax.axis_index("replica")
        self.c = self.rep % 2
        self.r = self.rep // 2
        self.bits = [(self.r // 2 ** (nbits - 1 - b)) % 2 for b in range(nbits)]
        self.over_x = (1 - self.s, self.rep)
        self.over_core = (self.s, self.rep + 1 - 2 * self.c)
        self.diagonal = (1 - self.s, self.rep + 1 - 2 * self.c)

    def over_bit(self, b):
        return (self.s, self.rep + (1 - 2 * self.bits[b]) * 2 ** (self.nbits - b))

    def peers(self):
        return [self.over_x, self.over_core, self.diagonal] + [
            self.over_bit(b) for b in range(self.nbits)
        ]

    def barrier(self):
        sem = pltpu.get_barrier_semaphore()
        for peer in self.peers():
            pl.semaphore_signal(sem, inc=1, device_id=peer, device_id_type=MESH)
        pl.semaphore_wait(sem, 3 + self.nbits)


class Mover:
    def __init__(self, send, recv, local):
        self.send, self.recv, self.local_sems = send, recv, local
        self.n = self.m = 0
        self.sent = []

    def remote(self, src, dst, peer):
        one = pltpu.make_async_remote_copy(
            src_ref=src,
            dst_ref=dst,
            send_sem=self.send.at[self.n],
            recv_sem=self.recv.at[self.n],
            device_id=peer,
            device_id_type=MESH,
        )
        self.n += 1
        one.start()
        self.sent.append(one)
        return one

    def local(self, src, dst):
        one = pltpu.make_async_copy(src, dst, self.local_sems.at[self.m])
        self.m += 1
        one.start()
        return one

    def finish(self):
        for one in self.sent:
            one.wait_send()


def arrived(copies):
    for one in copies:
        one.wait_recv()


def pipe(body, grid, ins, outs):
    pltpu.emit_pipeline(
        body,
        grid=grid,
        in_specs=[
            pl.BlockSpec(v[1], v[2], pipeline_mode=pl.Buffered(1 if len(v) > 3 else 2)) for v in ins
        ],
        out_specs=[pl.BlockSpec(b, m) for _, b, m in outs],
    )(*[v[0] for v in ins], *[r for r, _, _ in outs])


def ds(start, size, step=None):
    return pl.ds(pl.multiple_of(start, step or size), size)


def normalize(x, sm, width):
    mean = jnp.mean(x, axis=1, keepdims=True)
    center = x - mean
    spread = jnp.mean(center * center, axis=1, keepdims=True)
    rstd = lax.rsqrt(spread + EPSILON)
    n = center * rstd
    one = (n * sm[:, pl.ds(0, width)] + sm[:, pl.ds(width, width)]).astype(BF)
    two = (n * sm[:, pl.ds(2 * width, width)] + sm[:, pl.ds(3 * width, width)]).astype(BF)
    lane = lax.broadcasted_iota(jnp.int32, (x.shape[0], 128), 1)
    return one, two, jnp.where(lane == 0, mean, rstd)


class Reduce:
    def __init__(self, me, mv, g, order, got, sums, ahead):
        self.me, self.mv, self.g, self.order = me, mv, g, order
        self.got, self.sums, self.ahead = got, sums, ahead
        self.step = 0
        self.flying = None
        self.fetched = []

    def at(self, level, step, last):
        gone = self.order[:level]
        out = []
        for b in range(self.me.nbits):
            if b in gone:
                continue
            if b in self.order[:step]:
                out.append(self.me.bits[b])
            elif step < len(self.order) and b == self.order[step]:
                out.append(last)
            else:
                out.append(slice(None))
        return tuple(out)

    def go(self):
        k = self.step
        if self.flying is not None:
            self.flying.wait_recv()
        b = self.order[k]
        other = 1 - self.me.bits[b]
        if k == 0:
            src = self.g.at[self.at(0, 0, other)]
        elif k == 1:
            src = self.sums[0]
            add_up([self.g.at[self.at(0, 1, other)], self.got[0].at[self.at(1, 1, other)]], src)
            for t in range(2, self.me.nbits + 1):
                last = 1 - self.me.bits[self.order[t]] if t < self.me.nbits else None
                for level, ref in ((0, self.g), (1, self.got[0])):
                    self.fetched.append(
                        self.mv.local(ref.at[self.at(level, t, last)], self.ahead[t - 2].at[level])
                    )
        else:
            src = self.sums[k - 1]
            self.total(k, other, src)
        self.flying = self.mv.remote(src, self.got[k], self.me.over_bit(b))
        self.step += 1

    def total(self, k, last, out):
        for one in self.fetched[2 * (k - 2) : 2 * (k - 1)]:
            one.wait()
        near = self.ahead[k - 2]
        later = [self.got[j - 1].at[self.at(j, k, last)] for j in range(2, k + 1)]
        lead = out.shape[:-2]
        rows = out.shape[-2]
        for m in range(2 ** len(lead)):
            at = tuple((m // 2 ** (len(lead) - 1 - i)) % 2 for i in range(len(lead)))
            value = near[(0,) + at].astype(F32) + near[(1,) + at].astype(F32)
            for one in later:
                value = value + one[at].astype(F32)
            out[at] = value.astype(out.dtype)

    def end(self, out):
        self.flying.wait_recv()
        self.total(self.me.nbits, None, out)


def add_up(sources, out):
    shape = sources[0].shape
    lead = shape[:-2]
    split = 2 if len(lead) < 2 else 1
    block = (1,) * len(lead) + (shape[-2] // split, shape[-1])

    def body(*refs):
        total = refs[0][...].astype(F32)
        for one in refs[1:-1]:
            total = total + one[...].astype(F32)
        refs[-1][...] = total.astype(refs[-1].dtype)

    index = lambda *g: g + (0,)
    pipe(body, lead + (split,), [(v, block, index) for v in sources], [(out, block, index)])


def attention_body(acc_k, acc_v, packed, gctx, tab, ctx_out, grad_out, sums):
    rows, width = gctx.shape[1:]
    t = tab[0]
    lane = lax.broadcasted_iota(jnp.int32, (rows, 128), 1)
    quart = ROT // 2
    cos = jnp.where(lane < quart, t, jnp.where(lane < ROT, pltpu.roll(t, quart, 1), 1.0))
    sin = jnp.where(lane < quart, -pltpu.roll(t, 128 - quart, 1), jnp.where(lane < ROT, t, 0.0))

    def rotate(v, at, sign):
        low = v[:, :128]
        swapped = jnp.where(
            lane[at] < quart, pltpu.roll(low, 128 - quart, 1), pltpu.roll(low, quart, 1)
        )
        return jnp.concatenate([low * cos[at] + swapped * (sign * sin[at]), v[:, 128:]], axis=1)

    ids_row = t.T[ROT : ROT + 1, :]
    inv_root = HEAD ** (-0.5)
    part = rows // 2
    every = slice(None)
    for h in range(width // HEAD):
        cq = pl.ds(h * HEAD, HEAD)
        ck = pl.ds(width + h * HEAD, HEAD)
        cv = pl.ds(2 * width + h * HEAD, HEAD)
        q = rotate(packed[0, :, cq], every, 1.0).astype(BF)
        k = rotate(packed[0, :, ck], every, 1.0).astype(BF)
        v = packed[0, :, cv].astype(BF)
        sum_q = None
        for p in range(2):
            at = slice(p * part, (p + 1) * part)
            keys = (p + 1) * part
            row = p * part + lax.broadcasted_iota(jnp.int32, (part, keys), 0)
            col = lax.broadcasted_iota(jnp.int32, (part, keys), 1)
            allowed = (t[at, ROT : ROT + 1] == ids_row[:, :keys]) & (col <= row)
            g = gctx[0, at, cq]
            scores = jnp.where(allowed, dot(q[at], k[:keys], 1, 1) * inv_root, NEG_FILL)
            peak = jnp.max(scores, axis=1, keepdims=True)
            e = jnp.exp(scores - peak)
            total = jnp.sum(e, axis=1, keepdims=True)
            probs = e * (1.0 / total)
            probs_b = probs.astype(BF)
            context = dot(probs_b, v[:keys], 1, 0)
            ctx_out[0, at, cq] = context.astype(BF)
            row_dot = jnp.sum(g.astype(F32) * context, axis=1, keepdims=True)
            grad_probs = dot(g, v[:keys], 1, 1)
            grad_scores = (probs * (grad_probs - row_dot) * inv_root).astype(BF)
            gq = rotate(dot(grad_scores, k[:keys], 1, 0), at, -1.0)
            grad_out[0, at, cq] = gq.astype(BF)
            one = jnp.sum(gq, axis=0, keepdims=True)
            sum_q = one if sum_q is None else sum_q + one
            gk = dot(grad_scores, q[at], 0, 0)
            gv = dot(probs_b, g, 0, 0)
            if p == 0:
                acc_k[:keys], acc_v[:keys] = gk, gv
            else:
                acc_k[:part] += gk[:part]
                acc_v[:part] += gv[:part]
                acc_k[part:keys], acc_v[part:keys] = gk[part:], gv[part:]
        gk = rotate(acc_k[...], every, -1.0)
        gv = acc_v[...]
        grad_out[0, :, ck] = gk.astype(BF)
        grad_out[0, :, cv] = gv.astype(BF)
        sums[0, :, cq] = jnp.broadcast_to(sum_q, (8, HEAD))
        sums[0, :, ck] = jnp.broadcast_to(jnp.sum(gk, axis=0, keepdims=True), (8, HEAD))
        sums[0, :, cv] = jnp.broadcast_to(jnp.sum(gv, axis=0, keepdims=True), (8, HEAD))


def gelu_and_slope(a):
    half_erf = 0.5 * lax.erf(a * 0.7071067811865476)
    cdf = 0.5 + half_erf
    slope = cdf + a * (jnp.exp(-0.5 * a * a) * 0.3989422804014327)
    return a * cdf, slope


def step_kernel(nbits, names, *refs):
    r = dict(zip(names, refs, strict=True))
    hid, cot, tab, small = r["hid"], r["cot"], r["tab"], r["small"]
    wqkv, wdense, wfc1, wfc2 = r["wqkv"], r["wdense"], r["wfc1"], r["wfc2"]
    xall, call, tall = r["xall"], r["call"], r["tall"]
    n1, n2, st = r["n1"], r["n2"], r["st"]
    gctx, gact, act, gpre, fsum = r["gctx"], r["gact"], r["act"], r["gpre"], r["fsum"]
    packed, ctx, gpk, qsum = r["packed"], r["ctx"], r["gpk"], r["qsum"]
    outp, outr, outx = r["outp"], r["outr"], r["outx"]
    up, ur, ux, usum = r["up"], r["ur"], r["ux"], r["usum"]
    wq, wf1, wf2, wd = r["wq"], r["wf1"], r["wf2"], r["wd"]
    sm_own, sm_got, sm = r["sm_own"], r["sm_got"], r["sm"]

    me = Place(nbits)
    s, c = me.s, me.c
    rows, width = hid.shape
    half = width // 2
    quarter = width // 4
    ffq = wf2.shape[0]
    mine = tuple(me.bits)
    every = (slice(None),) * (nbits + 1)
    mv = Mover(r["send"], r["recv"], r["lsem"])
    near, far = pl.ds(0, 2), pl.ds(2, 2)

    bring = [
        mv.local(small, sm_own),
        mv.local(wfc2.at[ds(c * ffq, ffq)], wf2),
        mv.local(wdense.at[ds(c * quarter, quarter)], wd),
    ]
    bring_w = [mv.local(wfc1.at[every + (ds((2 * s + c) * ffq, ffq),)], wf1.at[s])] + [
        mv.local(
            wqkv.at[every + (ds(g * width + (2 * s + c) * quarter, quarter),)],
            wq.at[(s,) + every + (pl.ds(g * quarter, quarter),)],
        )
        for g in range(3)
    ]
    me.barrier()

    away = 2 * (1 - s) + c
    x_small = mv.remote(small, sm_got, me.over_x)
    x_q = [
        mv.remote(
            wqkv.at[mine + (slice(None), ds(g * width + away * quarter, quarter))],
            wq.at[(s,) + mine + (slice(None), pl.ds(g * quarter, quarter))],
            me.over_x,
        )
        for g in range(3)
    ]
    x_f1 = mv.remote(
        wfc1.at[mine + (slice(None), ds(away * ffq, ffq))], wf1.at[(s,) + mine], me.over_x
    )
    c_cot = mv.remote(cot, call.at[1], me.over_core)
    c_hid = mv.remote(hid, xall.at[1], me.over_core)
    c_tab = mv.remote(tab, tall.at[1], me.over_core)

    last_bit = nbits - 1

    class Spread:
        def __init__(self, w, first):
            self.w, self.flying, self.final, self.b = w, first, [], 0

        def go(self):
            arrived(self.flying)
            self.flying = []
            b = self.b
            if b < last_bit:
                at = tuple(slice(None) if k < b else me.bits[k] for k in range(nbits))
                self.flying.append(
                    mv.remote(self.w.at[(1 - s,) + at], self.w.at[(1 - s,) + at], me.over_bit(b))
                )
            at = tuple(
                slice(None) if k < b - 1 else (1 - me.bits[k] if k == b - 1 else me.bits[k])
                for k in range(nbits)
            )
            self.final.append(
                mv.remote(self.w.at[(1 - s,) + at], self.w.at[(1 - s,) + at], me.over_bit(last_bit))
            )
            self.b += 1

        def done(self):
            while self.b <= last_bit:
                self.go()
            arrived(self.final)

    acc, got = r["acc"], r["got"]
    acc[0] = jnp.zeros(acc.shape[1:], F32)

    def stage(own_x, own_c, own_t):
        pairs = ((hid, own_x, xall.at[0]), (cot, own_c, call.at[0]), (tab, own_t, tall.at[0]))
        for one in [mv.local(a, b) for a, b, _ in pairs]:
            one.wait()
        out = [mv.local(b, o) for _, b, o in pairs]
        acc[0, 4:5, :] = jnp.sum(own_c[...].astype(F32), axis=0, keepdims=True)
        for one in out:
            one.wait()

    pl.run_scoped(
        stage,
        pltpu.VMEM((rows, width), BF),
        pltpu.VMEM((rows, width), BF),
        pltpu.VMEM((rows, 128), F32),
    )
    for one in bring:
        one.wait()

    tile = min(512, ffq)
    sub = rows // 2
    tok2 = lambda i, j: (i, j, 0)

    def from_cot(at):
        def body(a, o, ob):
            for k in range(ffq // tile):
                cols = pl.ds(k * tile, tile)
                o[0, :, cols] = dot(a[0], wf2[cols, :], 1, 1)
            ob[0] = dot(a[0], wd[...], 1, 1).astype(BF)

        pipe(
            body,
            (2, 2),
            [(call.at[at], (1, sub, width), tok2)],
            [(gact.at[at], (1, sub, ffq), tok2), (gctx.at[at], (1, sub, quarter), tok2)],
        )

    def from_cot_after(at):
        def body(a, slope, o, ob, o_sum):
            for k in range(ffq // tile):
                cols = pl.ds(k * tile, tile)
                grad = dot(a[0], wf2[cols, :], 1, 1) * slope[0, :, cols]
                o[0, :, cols] = grad.astype(BF)
                o_sum[0, :, cols] = jnp.broadcast_to(
                    jnp.sum(grad, axis=0, keepdims=True), (8, tile)
                )
            ob[0] = dot(a[0], wd[...], 1, 1).astype(BF)

        pipe(
            body,
            (2, 2),
            [(call.at[at], (1, sub, width), tok2), (gact.at[at], (1, sub, ffq), tok2)],
            [
                (gpre.at[at], (1, sub, ffq), tok2),
                (gctx.at[at], (1, sub, quarter), tok2),
                (fsum.at[at], (1, 8, ffq), tok2),
            ],
        )

    def norm_blocks(at):
        def body(x, o1, o2, ost):
            o1[0], o2[0], ost[0] = normalize(x[0].astype(F32), sm, width)

        pipe(
            body,
            (2, 2),
            [(xall.at[at], (1, sub, width), tok2)],
            [
                (n1.at[at], (1, sub, width), tok2),
                (n2.at[at], (1, sub, width), tok2),
                (st.at[at], (1, sub, 128), tok2),
            ],
        )

    bias_q = lambda g: sm[:, ds(4 * width + g * width + (2 * s + c) * quarter, quarter)]
    bias_f = lambda k: sm[:, ds(7 * width + (2 * s + c) * ffq + k * tile, tile)]
    all_rows = (slice(None),) + every

    def hidden_units(at):
        def body(a, g, o_act, o_pre, o_sum):
            for k in range(ffq // tile):
                cols = pl.ds(k * tile, tile)
                pre = dot(a[0], flat(wf1[all_rows + (cols,)]), 1, 0) + bias_f(k)
                value, slope = gelu_and_slope(pre)
                o_act[0, :, cols] = value.astype(BF)
                grad = g[0, :, cols] * slope
                o_pre[0, :, cols] = grad.astype(BF)
                o_sum[0, :, cols] = jnp.broadcast_to(
                    jnp.sum(grad, axis=0, keepdims=True), (8, tile)
                )

        pipe(
            body,
            (2, 2),
            [(n2.at[at], (1, sub, width), tok2), (gact.at[at], (1, sub, ffq), tok2)],
            [
                (act.at[at], (1, sub, ffq), tok2),
                (gpre.at[at], (1, sub, ffq), tok2),
                (fsum.at[at], (1, 8, ffq), tok2),
            ],
        )

    def forward(at):
        def body(one, two, o_act, o_slope, o_packed):
            for k in range(ffq // tile):
                cols = pl.ds(k * tile, tile)
                pre = dot(two[0], flat(wf1[all_rows + (cols,)]), 1, 0) + bias_f(k)
                value, slope = gelu_and_slope(pre)
                o_act[0, :, cols] = value.astype(BF)
                o_slope[0, :, cols] = slope
            for g in range(3):
                cols = pl.ds(g * quarter, quarter)
                o_packed[0, :, cols] = dot(one[0], flat(wq[all_rows + (cols,)]), 1, 0) + bias_q(g)

        pipe(
            body,
            (2, 2),
            [(n1.at[at], (1, sub, width), tok2), (n2.at[at], (1, sub, width), tok2)],
            [
                (act.at[at], (1, sub, ffq), tok2),
                (gact.at[at], (1, sub, ffq), tok2),
                (packed.at[at], (1, sub, 3 * quarter), tok2),
            ],
        )

    def project(at):
        def body(a, o):
            for g in range(3):
                cols = pl.ds(g * quarter, quarter)
                o[0, :, cols] = dot(a[0], flat(wq[all_rows + (cols,)]), 1, 0) + bias_q(g)

        pipe(
            body,
            (2, 2),
            [(n1.at[at], (1, sub, width), tok2)],
            [(packed.at[at], (1, sub, 3 * quarter), tok2)],
        )

    def attend(at):
        whole = lambda i: (i, 0, 0)
        pipe(
            partial(attention_body, r["acc_k"], r["acc_v"]),
            (2,),
            [
                (packed.at[at], (1, rows, 3 * quarter), whole),
                (gctx.at[at], (1, rows, quarter), whole),
                (tall.at[at], (1, rows, 128), whole),
            ],
            [
                (ctx.at[at], (1, rows, quarter), whole),
                (gpk.at[at], (1, rows, 3 * quarter), whole),
                (qsum.at[at], (1, 8, 3 * quarter), whole),
            ],
        )

    def finish(at, plus=None):
        def body(*refs):
            a, b, ga, gb, x, stat = refs[:6]
            o, ou, osum = refs[-3:]
            for k in range(4):
                cols = pl.ds(k * quarter, quarter)
                value = dot(a[0], wd[:, cols], 1, 0) + dot(b[0], wf2[:, cols], 1, 0)
                if plus is not None:
                    value = value + refs[6][0, :, cols].astype(F32)
                o[0, :, cols] = value.astype(BF)
            mean, rstd = stat[0, :, 0:1], stat[0, :, 1:2]
            for k in range(4):
                cols = pl.ds(k * quarter, quarter)
                one = dot(ga[0], flat(wq[k // 2, k % 2]), 1, 1)
                two = dot(gb[0], flat(wf1[k // 2, k % 2]), 1, 1)
                n = (x[0, :, cols].astype(F32) - mean) * rstd
                value = (
                    one * sm[:, pl.ds(k * quarter, quarter)]
                    + two * sm[:, pl.ds(2 * width + k * quarter, quarter)]
                )
                if plus is not None:
                    value = value + refs[7][0, :, cols].astype(F32)
                ou[0, :, cols] = value.astype(BF)
                osum[0, 0:1, cols] = jnp.sum(one * n, axis=0, keepdims=True)
                osum[0, 1:2, cols] = jnp.sum(one, axis=0, keepdims=True)
                osum[0, 2:3, cols] = jnp.sum(two * n, axis=0, keepdims=True)
                osum[0, 3:4, cols] = jnp.sum(two, axis=0, keepdims=True)

        pipe(
            body,
            (at.size, 2),
            [
                (ctx.at[at], (1, sub, quarter), tok2),
                (act.at[at], (1, sub, ffq), tok2),
                (gpk.at[at], (1, sub, 3 * quarter), tok2),
                (gpre.at[at], (1, sub, ffq), tok2),
                (xall.at[at], (1, sub, width), tok2),
                (st.at[at], (1, sub, 128), tok2),
            ]
            + [(v, (1, sub, width), tok2) for v in plus or ()],
            [
                (outp.at[at], (1, sub, width), tok2),
                (up.at[at], (1, sub, width), tok2),
                (usum.at[at], (1, 8, width), tok2),
            ],
        )

    def row_grad(lhs, keep, send, first, cols_tile, count):
        per_owner = keep.shape[-2]
        dims = keep.shape[:-2]
        lw = lhs.shape[2]

        def body(a, b, o_keep, o_send):
            full = dot(flat(a[...]), flat(b[...]), 0, 0).astype(BF)
            full = full.reshape((lw // (2 * per_owner), 2, per_owner, full.shape[-1]))
            zero, one = full[:, 0], full[:, 1]
            o_keep[...] = jnp.where(c == 0, zero, one).reshape(o_keep.shape)
            o_send[...] = jnp.where(c == 0, one, zero).reshape(o_send.shape)

        block = dims + (per_owner, cols_tile)
        at = lambda j: (0,) * (len(dims) + 1) + (j,)
        pipe(
            body,
            (count,),
            [
                (lhs, (4, rows, lw), lambda j: (0, 0, 0), True),
                (call, (4, rows, cols_tile), lambda j: (0, 0, first + j)),
            ],
            [(keep, block, at), (send, block, at)],
        )

    def column_grad(lhs, rhs, out, first):
        block = (1,) + out.shape[1:]

        def body(a, b, o):
            o[...] = dot(flat(a[...]), flat(b[...]), 0, 0).astype(BF).reshape(block)

        pipe(
            body,
            (2,),
            [
                (lhs, (4, rows, quarter), lambda j: (0, 0, first + j)),
                (rhs, (4, rows, rhs.shape[2]), lambda j: (0, 0, 0), True),
            ],
            [(out, block, lambda j: (j,) + (0,) * (len(block) - 1))],
        )

    usual = tuple(reversed(range(nbits)))
    swapped = (usual[1], usual[0]) + usual[2:] if nbits > 1 else usual

    def reduction(name, g, order):
        return Reduce(
            me,
            mv,
            g,
            order,
            [r[f"{name}_got{t}"] for t in range(nbits)],
            [r[f"{name}_sum{t}"] for t in range(1, nbits)],
            [r[f"{name}_ahead{t}"] for t in range(2, nbits + 1)],
        )

    f1 = Spread(wf1, [x_f1])
    q = Spread(wq, x_q)
    q.go()
    x_f1.wait_recv()
    f1.flying = []
    x_hid = mv.remote(hid, xall.at[2], me.over_x)
    c_cot.wait_recv()
    from_cot(near)
    x_small.wait_recv()
    lo = 0
    for n in (half, half, half, half, 3 * half, ffq * 2, half, half):
        sm[:, ds(2 * lo + s * n, n, 128)] = sm_own[:, pl.ds(lo, n)]
        sm[:, ds(2 * lo + (1 - s) * n, n, 128)] = sm_got[:, pl.ds(lo, n)]
        lo += n
    arrived([c_hid, c_tab])
    norm_blocks(near)
    q.go()
    f1.go()
    for one in bring_w:
        one.wait()
    for _ in range(2, nbits):
        q.go()
        f1.go()
    x_hid.wait_recv()
    d_hid = mv.remote(xall.at[2], xall.at[3], me.over_core)
    x_cot = mv.remote(cot, call.at[2], me.over_x)
    while f1.b <= last_bit:
        f1.go()
    d_hid.wait_recv()
    norm_blocks(far)
    q.done()
    project(near)
    attend(near)
    f1.done()
    hidden_units(near)
    x_cot.wait_recv()
    d_cot = mv.remote(call.at[2], call.at[3], me.over_core)
    x_tab = mv.remote(tab, tall.at[2], me.over_x)
    forward(far)
    d_cot.wait_recv()

    f2a, f2b, f2a_s, f2b_s = r["f2a"], r["f2b"], r["f2a_send"], r["f2b_send"]
    row_grad(act, f2a.at[c], f2a_s, 0, 512, width // 1024)
    f2a_swap = mv.remote(f2a_s, f2a.at[c], me.over_core)
    row_grad(act, f2b.at[c], f2b_s, width // 1024, 512, width // 1024)
    f2b_swap = mv.remote(f2b_s, f2b.at[c], me.over_core)
    f2a_swap.wait_recv()
    red_f2a = reduction("f2a", f2a, usual)
    red_f2a.go()
    x_tab.wait_recv()
    d_tab = mv.remote(tall.at[2], tall.at[3], me.over_core)
    from_cot_after(far)
    f2b_swap.wait_recv()
    red_f2b = reduction("f2b", f2b, usual)
    red_f2b.go()
    g1 = r["g1"]
    column_grad(n2, gpre, g1.at[0], 0)
    red_f1a = reduction("f1a", g1.at[0], swapped)
    red_f1a.go()
    column_grad(n2, gpre, g1.at[1], 2)
    red_f1b = reduction("f1b", g1.at[1], usual)
    red_f1b.go()

    d_tab.wait_recv()
    attend(far)
    red_f2a.go()
    gq = r["gq"]
    column_grad(n1, gpk, gq.at[0], 0)
    red_qa = reduction("qa", gq.at[0], usual)
    red_qa.go()
    column_grad(n1, gpk, gq.at[1], 2)
    red_qb = reduction("qb", gq.at[1], swapped)
    red_qb.go()
    red_f2b.go()
    d = r["d"]
    row_grad(ctx, d.at[c], r["d_send"], 0, 512, width // 512)
    d_swap = mv.remote(r["d_send"], d.at[c], me.over_core)
    red_f1a.go()
    d_swap.wait_recv()
    red_d = reduction("d", d, usual)
    red_d.go()

    finish(pl.ds(3, 1))
    o_far = mv.remote(outp.at[3], outr.at[1], me.over_core)
    u_far = mv.remote(up.at[3], ur.at[1], me.over_core)
    red_f1b.go()
    red_qb.go()
    red_f2a.go()
    arrived([o_far, u_far])
    finish(pl.ds(2, 1), (outr.at[pl.ds(1, 1)], ur.at[pl.ds(1, 1)]))
    o_x = mv.remote(outp.at[2], outx, me.over_x)
    u_x = mv.remote(up.at[2], ux, me.over_x)
    red_qa.go()
    red_d.go()
    red_f2b.go()
    red_f1a.go()
    finish(pl.ds(1, 1))
    u_near = mv.remote(up.at[1], ur.at[0], me.over_core)
    o_near = mv.remote(outp.at[1], outr.at[0], me.over_core)
    red_f1b.go()
    red_qb.go()
    red_qa.go()
    red_d.go()
    finish(pl.ds(0, 1))

    sums_in = [
        mv.local(usum, r["usum_v"]),
        mv.local(qsum, r["qsum_v"]),
        mv.local(fsum, r["fsum_v"]),
    ]
    for one in sums_in:
        one.wait()
    acc[0, 0:4, :] = jnp.sum(r["usum_v"][:, 0:4, :] + r["usum_v"][:, 8:12, :], axis=0)
    for g in range(3):
        acc[0, 5 + g : 6 + g, ds((2 * s + c) * quarter, quarter)] = jnp.sum(
            r["qsum_v"][:, 0:1, pl.ds(g * quarter, quarter)], axis=0
        )
    f_row = jnp.sum(r["fsum_v"][:, 0:1, :] + r["fsum_v"][:, 8:9, :], axis=0)
    acc[0, 8:9, ds(c * ffq, ffq)] = jnp.where(s == 0, f_row, 0.0)
    acc[0, 9:10, ds(c * ffq, ffq)] = jnp.where(s == 0, 0.0, f_row)
    small_peers = [me.over_x, me.over_core] + [me.over_bit(b) for b in range(nbits)]
    small_step = [0, None]

    def small_go():
        k, flying = small_step
        if k > len(small_peers):
            return
        if flying is not None:
            flying.wait_recv()
            acc[k] = acc[k - 1] + got[k - 1]
        if k < len(small_peers):
            small_step[1] = mv.remote(acc.at[k], got.at[k], small_peers[k])
        else:
            r["tot"][...] = acc[k]
        small_step[0] = k + 1

    small_go()
    reds = (red_f2a, red_f2b, red_f1a, red_f1b, red_qa, red_d, red_qb)
    for _ in range(nbits):
        for one in reds:
            if one.step < nbits:
                one.go()
                small_go()

    tok = lambda i: (i, 0)
    quarter_rows = rows // 4
    o_near.wait_recv()
    o_x.wait_recv()

    def result_body(x, a, b, e, o):
        o[...] = (
            x[...].astype(F32)
            + (
                a[...].astype(F32)
                + b[...].astype(F32)
                + e[...].astype(F32)
                + (sm[:, pl.ds(9 * width, width)] + sm[:, pl.ds(10 * width, width)])
            )
        ).astype(BF)

    block = (quarter_rows, width)
    pipe(
        result_body,
        (4,),
        [(v, block, tok) for v in (hid, outp.at[0], outr.at[0], outx)],
        [(r["result"], block, tok)],
    )
    u_near.wait_recv()
    u_x.wait_recv()

    def grad_body(x, y, a, b, e, stat, o):
        u = a[...].astype(F32) + b[...].astype(F32) + e[...].astype(F32)
        mean, rstd = stat[:, 0:1], stat[:, 1:2]
        n = (x[...].astype(F32) - mean) * rstd
        o[...] = y[...].astype(F32) + rstd * (
            u - jnp.mean(u, axis=1, keepdims=True) - n * jnp.mean(u * n, axis=1, keepdims=True)
        )

    pipe(
        grad_body,
        (4,),
        [(v, block, tok) for v in (hid, cot, up.at[0], ur.at[0], ux)]
        + [(st.at[0], (quarter_rows, 128), tok)],
        [(r["grad"], block, tok)],
    )
    small_go()

    last = []

    def hand_over(e, got):
        last.append(mv.remote(e.at[s, 1 - c], got.at[0], me.over_core))
        last.append(mv.remote(e.at[1 - s, c], got.at[1], me.over_x))
        last.append(mv.remote(e.at[1 - s, 1 - c], got.at[2], me.diagonal))

    e_f1, e_q, r_f1, r_q = r["e_f1"], r["e_q"], r["r_f1"], r["r_q"]
    for red, e, k, tmp in ((red_f1a, e_f1, 0, "end_f"), (red_f1b, e_f1, 1, "end_f")):
        red.end(r[tmp])
        e[k] = r[tmp][...].reshape(e.shape[1:])
    hand_over(e_f1, r_f1)
    red_f2a.end(r["o_f2"].at[:, pl.ds(0, half)])
    red_f2b.end(r["o_f2"].at[:, pl.ds(half, half)])
    red_d.end(r["o_d"])
    for red, e, k, tmp in ((red_qa, e_q, 0, "end_q"), (red_qb, e_q, 1, "end_q")):
        red.end(r[tmp])
        e[k] = r[tmp][...].reshape(e.shape[1:])
    hand_over(e_q, r_q)
    for _ in range(nbits + 3):
        small_go()
    arrived(last)
    places = ((s, c), (s, 1 - c), (1 - s, c), (1 - s, 1 - c))
    for k, (ps, pc) in enumerate(places):
        part_f = e_f1[s, c] if k == 0 else r_f1[k - 1]
        r["o_f1"][:, ds((2 * ps + pc) * ffq, ffq)] = part_f.astype(F32)
        for g in range(3):
            cols = pl.ds(g * quarter, quarter)
            part_q = e_q[s, c, :, cols] if k == 0 else r_q[k - 1, :, cols]
            r["o_q"][:, ds(g * width + (2 * ps + pc) * quarter, quarter)] = part_q.astype(F32)
    mv.finish()


def step(nbits, hid, cot, tab, small, wqkv, wdense, wfc1, wfc2):
    rows, width = hid.shape
    half, ff = wfc1.shape
    quarter, ffq = width // 4, ff // 4
    groups = 2**nbits
    own_rows = half // groups
    half_own = own_rows // 2
    per_ff = ffq // groups
    length = small.shape[1]
    bits = (2,) * nbits
    hbm, vmem = pl.BlockSpec(memory_space=pl.ANY), pl.BlockSpec(memory_space=pltpu.VMEM)
    sds = jax.ShapeDtypeStruct
    outs = {
        "result": (hbm, (rows, width), BF),
        "grad": (hbm, (rows, width), F32),
        "o_f2": (vmem, (per_ff, width), F32),
        "o_d": (vmem, (half_own, width), F32),
        "o_f1": (vmem, (half_own, ff), F32),
        "o_q": (vmem, (half_own, 3 * width), F32),
        "tot": (vmem, (16, width), F32),
        "xall": (hbm, (4, rows, width), BF),
        "call": (hbm, (4, rows, width), BF),
        "tall": (hbm, (4, rows, 128), F32),
        "n1": (hbm, (4, rows, width), BF),
        "n2": (hbm, (4, rows, width), BF),
        "st": (hbm, (4, rows, 128), F32),
        "gctx": (hbm, (4, rows, quarter), BF),
        "gact": (hbm, (4, rows, ffq), F32),
        "act": (hbm, (4, rows, ffq), BF),
        "gpre": (hbm, (4, rows, ffq), BF),
        "fsum": (hbm, (4, 16, ffq), F32),
        "packed": (hbm, (4, rows, 3 * quarter), F32),
        "ctx": (hbm, (4, rows, quarter), BF),
        "gpk": (hbm, (4, rows, 3 * quarter), BF),
        "qsum": (hbm, (4, 8, 3 * quarter), F32),
        "f2a": (hbm, bits + (per_ff, half), BF),
        "f2b": (hbm, bits + (per_ff, half), BF),
        "f2a_send": (hbm, bits[1:] + (per_ff, half), BF),
        "f2b_send": (hbm, bits[1:] + (per_ff, half), BF),
        "g1": (hbm, (2,) + bits + (own_rows, ffq), BF),
        "d": (hbm, bits + (half_own, width), BF),
        "d_send": (hbm, bits[1:] + (half_own, width), BF),
        "gq": (hbm, (2,) + bits + (own_rows, 3 * quarter), BF),
        "outp": (hbm, (4, rows, width), BF),
        "outr": (hbm, (2, rows, width), BF),
        "outx": (hbm, (rows, width), BF),
        "up": (hbm, (4, rows, width), BF),
        "ur": (hbm, (2, rows, width), BF),
        "ux": (hbm, (rows, width), BF),
        "usum": (hbm, (4, 16, width), F32),
    }
    extra = {}
    for name, tail in (
        ("f2a", (per_ff, half)),
        ("f2b", (per_ff, half)),
        ("f1a", (own_rows, ffq)),
        ("f1b", (own_rows, ffq)),
        ("d", (half_own, width)),
        ("qa", (own_rows, 3 * quarter)),
        ("qb", (own_rows, 3 * quarter)),
    ):
        for t in range(nbits):
            dims = (2,) * (nbits - 1 - t) + tail
            if t == 0:
                outs[f"{name}_got{t}"] = (hbm, dims, BF)
            else:
                extra[f"{name}_got{t}"] = pltpu.VMEM(dims, BF)
            if t == 1:
                outs[f"{name}_sum{t}"] = (hbm, dims, BF)
            if t > 1:
                extra[f"{name}_sum{t}"] = pltpu.VMEM(dims, BF)
        for t in range(2, nbits + 1):
            dims = (2,) * max(nbits - 1 - t, 0) + tail
            extra[f"{name}_ahead{t}"] = pltpu.VMEM((2,) + dims, BF)
    scratch = {
        "wq": pltpu.VMEM((2,) + bits + (own_rows, 3 * quarter), BF),
        "wf1": pltpu.VMEM((2,) + bits + (own_rows, ffq), BF),
        "wf2": pltpu.VMEM((ffq, width), BF),
        "wd": pltpu.VMEM((quarter, width), BF),
        "sm_own": pltpu.VMEM((1, length), F32),
        "sm_got": pltpu.VMEM((1, length), F32),
        "sm": pltpu.VMEM((1, 2 * length), F32),
        "acc_k": pltpu.VMEM((rows, HEAD), F32),
        "acc_v": pltpu.VMEM((rows, HEAD), F32),
        "usum_v": pltpu.VMEM((4, 16, width), F32),
        "qsum_v": pltpu.VMEM((4, 8, 3 * quarter), F32),
        "fsum_v": pltpu.VMEM((4, 16, ffq), F32),
        "acc": pltpu.VMEM((3 + nbits, 16, width), F32),
        "got": pltpu.VMEM((2 + nbits, 16, width), F32),
        "r_f1": pltpu.VMEM((3, half_own, ffq), BF),
        "r_q": pltpu.VMEM((3, half_own, 3 * quarter), BF),
        "e_f1": pltpu.VMEM((2, 2, half_own, ffq), BF),
        "e_q": pltpu.VMEM((2, 2, half_own, 3 * quarter), BF),
        "end_f": pltpu.VMEM((own_rows, ffq), BF),
        "end_q": pltpu.VMEM((own_rows, 3 * quarter), BF),
        "send": pltpu.SemaphoreType.DMA((36 + 12 * nbits,)),
        "recv": pltpu.SemaphoreType.DMA((36 + 12 * nbits,)),
        "lsem": pltpu.SemaphoreType.DMA((24 + 14 * nbits,)),
        **extra,
    }
    ins = ("hid", "cot", "tab", "small", "wqkv", "wdense", "wfc1", "wfc2")
    got = pl.pallas_call(
        partial(step_kernel, nbits, ins + tuple(outs) + tuple(scratch)),
        in_specs=[hbm] * len(ins),
        out_specs=[one[0] for one in outs.values()],
        out_shape=[sds(*one[1:]) for one in outs.values()],
        scratch_shapes=list(scratch.values()),
        compiler_params=pltpu.CompilerParams(
            collective_id=0, has_side_effects=True, vmem_limit_bytes=VMEM_LIMIT
        ),
        name="step",
    )(
        hid,
        cot,
        tab,
        small,
        wqkv.reshape(bits + (own_rows, 3 * width)),
        wdense,
        wfc1.reshape(bits + (own_rows, ff)),
        wfc2,
    )
    return got[:7]


def rotary_table(seg):
    rows = seg.shape[0]
    index = jnp.arange(rows, dtype=jnp.int32)
    same = seg[:, None] == seg[None, :]
    first = jnp.min(jnp.where(same, index[None, :], rows), axis=1)
    offset = (index - first).astype(F32)
    frequency = jnp.exp(-jnp.log(10000.0) * jnp.arange(0, ROT, 2).astype(F32) / ROT)
    angles = offset[:, None] * frequency[None, :]
    ids = jnp.broadcast_to(seg.astype(F32)[:, None], (rows, 128 - ROT))
    return jnp.concatenate([jnp.cos(angles), jnp.sin(angles), ids], axis=1)


def local(
    nbits,
    hidden_in,
    out_cotangent,
    segment_ids,
    ln1_gain,
    ln1_bias,
    qkv_weight,
    qkv_bias,
    dense_weight,
    dense_bias,
    ln2_gain,
    ln2_bias,
    fc1_weight,
    fc1_bias,
    fc2_weight,
    fc2_bias,
):
    me = lax.axis_index("shard") * 2 ** (nbits + 1) + lax.axis_index("replica")
    owners = 2 ** (nbits + 2)
    width = hidden_in.shape[1]
    vectors = (
        ln1_gain, ln1_bias, ln2_gain, ln2_bias, qkv_bias, fc1_bias, dense_bias, fc2_bias
    )
    length = sum(v.shape[0] for v in vectors)
    small, lo = 0.0, 0
    for v in vectors:
        n = v.shape[0]
        small = small + jnp.pad(v.astype(F32), (lo, length - lo - n))
        lo += n
    result, grad, o_f2, o_d, o_f1, o_q, tot = step(
        nbits,
        hidden_in,
        out_cotangent,
        rotary_table(segment_ids),
        small[None],
        qkv_weight,
        dense_weight,
        fc1_weight,
        fc2_weight,
    )

    def own(v):
        return lax.dynamic_index_in_dim(v.reshape(v.shape[:-1] + (owners, -1)), me, v.ndim - 1, False)

    five = own(tot[:5])
    b_qkv = own(tot[5:8].reshape(-1))
    b_fc1 = own(tot[8:10].reshape(-1))
    return (
        result, grad, five[0], five[1], o_q, b_qkv, o_d, five[4],
        five[2], five[3], o_f1, b_fc1, o_f2, five[4],
    )


def solution(mesh):
    both = ("shard", "replica")
    nbits = (mesh.shape["replica"] // 2).bit_length() - 1
    wide, token, vector, matrix = P(both, None), P(both), P("shard"), P("shard", None)
    return jax.shard_map(
        partial(local, nbits),
        mesh=mesh,
        in_specs=(wide, wide, token, vector, vector, matrix, vector, matrix, vector)
        + (vector, vector, matrix, vector, matrix, vector),
        out_specs=(wide, wide, token, token, wide, token, wide, token)
        + (token, token, wide, token, wide, token),
        check_vma=False,
    )
```

```python
from functools import partial

import jax
import jax.numpy as jnp
from jax import lax
from jax.experimental import pallas as pl
from jax.experimental.pallas import tpu as pltpu
from jax.sharding import PartitionSpec as P

HEADS = 8
HEAD = 256
ROT = 64
NEG_FILL = -1e30
EPSILON = 1e-05
BF = jnp.bfloat16
F32 = jnp.float32
MESH = pl.DeviceIdType.MESH
ANY = pl.BlockSpec(memory_space=pl.ANY)
VMEM_LIMIT = 127 << 19


def dot(a, b, da, db):
    return lax.dot_general(a, b, (((da,), (db,)), ((), ())), preferred_element_type=F32)


def flat(v):
    return v.reshape((-1, v.shape[-1]))


class Place:
    def __init__(self, nbits):
        self.nbits = nbits
        self.s = lax.axis_index("shard")
        self.rep = lax.axis_index("replica")
        self.c = self.rep % 2
        self.r = self.rep // 2
        self.bits = [(self.r // 2 ** (nbits - 1 - b)) % 2 for b in range(nbits)]
        self.over_x = (1 - self.s, self.rep)
        self.over_core = (self.s, self.rep + 1 - 2 * self.c)
        self.diagonal = (1 - self.s, self.rep + 1 - 2 * self.c)

    def over_bit(self, b):
        return (self.s, self.rep + (1 - 2 * self.bits[b]) * 2 ** (self.nbits - b))

    def peers(self):
        return [self.over_x, self.over_core, self.diagonal] + [
            self.over_bit(b) for b in range(self.nbits)
        ]

    def barrier(self):
        sem = pltpu.get_barrier_semaphore()
        for peer in self.peers():
            pl.semaphore_signal(sem, inc=1, device_id=peer, device_id_type=MESH)
        pl.semaphore_wait(sem, 3 + self.nbits)


class Mover:
    def __init__(self, send, recv, local):
        self.send, self.recv, self.local_sems = send, recv, local
        self.n = self.m = 0
        self.sent = []

    def remote(self, src, dst, peer):
        one = pltpu.make_async_remote_copy(
            src_ref=src,
            dst_ref=dst,
            send_sem=self.send.at[self.n],
            recv_sem=self.recv.at[self.n],
            device_id=peer,
            device_id_type=MESH,
        )
        self.n += 1
        one.start()
        self.sent.append(one)
        return one

    def local(self, src, dst):
        one = pltpu.make_async_copy(src, dst, self.local_sems.at[self.m])
        self.m += 1
        one.start()
        return one

    def finish(self):
        for one in self.sent:
            one.wait_send()


def arrived(copies):
    for one in copies:
        one.wait_recv()


def pipe(body, grid, ins, outs):
    pltpu.emit_pipeline(
        body,
        grid=grid,
        in_specs=[
            pl.BlockSpec(v[1], v[2], pipeline_mode=pl.Buffered(1 if len(v) > 3 else 2)) for v in ins
        ],
        out_specs=[pl.BlockSpec(b, m) for _, b, m in outs],
    )(*[v[0] for v in ins], *[r for r, _, _ in outs])


def ds(start, size, step=None):
    return pl.ds(pl.multiple_of(start, step or size), size)


def normalize(x, sm, width):
    mean = jnp.mean(x, axis=1, keepdims=True)
    center = x - mean
    spread = jnp.mean(center * center, axis=1, keepdims=True)
    rstd = lax.rsqrt(spread + EPSILON)
    n = center * rstd
    one = (n * sm[:, pl.ds(0, width)] + sm[:, pl.ds(width, width)]).astype(BF)
    two = (n * sm[:, pl.ds(2 * width, width)] + sm[:, pl.ds(3 * width, width)]).astype(BF)
    lane = lax.broadcasted_iota(jnp.int32, (x.shape[0], 128), 1)
    return one, two, jnp.where(lane == 0, mean, rstd)


def blocks_of(shape):
    lead = len(shape) - 2
    return [tuple((m // 2 ** (lead - 1 - i)) % 2 for i in range(lead)) for m in range(2**lead)]


class Reduce:
    def __init__(self, me, mv, g, order, got, sums, ahead, came):
        self.me, self.mv, self.g, self.order = me, mv, g, order
        self.got, self.sums, self.ahead, self.came = got, sums, ahead, came
        self.step = 0
        self.flying = None
        self.fetched = []

    def at(self, level, step, last):
        gone = self.order[:level]
        out = []
        for b in range(self.me.nbits):
            if b in gone:
                continue
            if b in self.order[:step]:
                out.append(self.me.bits[b])
            elif step < len(self.order) and b == self.order[step]:
                out.append(last)
            else:
                out.append(slice(None))
        return tuple(out)

    def go(self):
        k = self.step
        if self.flying is not None:
            self.flying.wait_recv()
        b = self.order[k]
        other = 1 - self.me.bits[b]
        if k == 0:
            src = self.g.at[self.at(0, 0, other)]
            if self.me.nbits > 1:
                last = 1 - self.me.bits[self.order[1]]
                self.first = self.mv.local(self.g.at[self.at(0, 1, last)], self.sums[0])
        elif k == 1:
            src = self.sums[0]
            came = self.mv.local(self.got[0].at[self.at(1, 1, other)], self.came)
            for t in range(2, self.me.nbits + 1):
                last = 1 - self.me.bits[self.order[t]] if t < self.me.nbits else None
                for level, ref in ((0, self.g), (1, self.got[0])):
                    self.fetched.append(
                        self.mv.local(ref.at[self.at(level, t, last)], self.ahead[t - 2].at[level])
                    )
            self.first.wait()
            came.wait()
            for at in blocks_of(src.shape):
                src[at] = (src[at].astype(F32) + self.came[at].astype(F32)).astype(src.dtype)
        else:
            src = self.sums[k - 1]
            self.total(k, other, src)
        self.flying = self.mv.remote(src, self.got[k], self.me.over_bit(b))
        self.step += 1

    def total(self, k, last, out):
        for one in self.fetched[2 * (k - 2) : 2 * (k - 1)]:
            one.wait()
        near = self.ahead[k - 2]
        later = [self.got[j - 1].at[self.at(j, k, last)] for j in range(2, k + 1)]
        for at in blocks_of(out.shape):
            value = near[(0,) + at].astype(F32) + near[(1,) + at].astype(F32)
            for one in later:
                value = value + one[at].astype(F32)
            out[at] = value.astype(out.dtype)

    def end(self, out):
        self.flying.wait_recv()
        self.total(self.me.nbits, None, out)


def attention_body(acc_k, acc_v, packed, project, normed, gctx, tab, ctx_out, grad_out, sums):
    project(normed, packed)
    rows, width = gctx.shape[1:]
    t = tab[0]
    lane = lax.broadcasted_iota(jnp.int32, (rows, 128), 1)
    quart = ROT // 2
    cos = jnp.where(lane < quart, t, jnp.where(lane < ROT, pltpu.roll(t, quart, 1), 1.0))
    sin = jnp.where(lane < quart, -pltpu.roll(t, 128 - quart, 1), jnp.where(lane < ROT, t, 0.0))

    def rotate(v, at, sign):
        low = v[:, :128]
        swapped = jnp.where(
            lane[at] < quart, pltpu.roll(low, 128 - quart, 1), pltpu.roll(low, quart, 1)
        )
        return jnp.concatenate([low * cos[at] + swapped * (sign * sin[at]), v[:, 128:]], axis=1)

    ids_row = t.T[ROT : ROT + 1, :]
    inv_root = HEAD ** (-0.5)
    part = rows // 2
    every = slice(None)
    allowed = []
    for p in range(2):
        keys = (p + 1) * part
        row = p * part + lax.broadcasted_iota(jnp.int32, (part, keys), 0)
        col = lax.broadcasted_iota(jnp.int32, (part, keys), 1)
        same = t[p * part : (p + 1) * part, ROT : ROT + 1] == ids_row[:, :keys]
        allowed.append(same & (col <= row))
    for h in range(width // HEAD):
        cq = pl.ds(h * HEAD, HEAD)
        ck = pl.ds(width + h * HEAD, HEAD)
        cv = pl.ds(2 * width + h * HEAD, HEAD)
        q = (rotate(packed[:, cq], every, 1.0) * inv_root).astype(BF)
        k = rotate(packed[:, ck], every, 1.0).astype(BF)
        k_scaled = (k.astype(F32) * inv_root).astype(BF)
        v = packed[:, cv].astype(BF)
        sum_q = None
        for p in range(2):
            at = slice(p * part, (p + 1) * part)
            keys = (p + 1) * part
            g = gctx[0, at, cq]
            scores = jnp.where(allowed[p], dot(q[at], k[:keys], 1, 1), NEG_FILL)
            peak = jnp.max(scores, axis=1, keepdims=True)
            e = jnp.exp(scores - peak)
            total = jnp.sum(e, axis=1, keepdims=True)
            probs = e * (1.0 / total)
            probs_b = probs.astype(BF)
            context = dot(probs_b, v[:keys], 1, 0)
            ctx_out[0, at, cq] = context.astype(BF)
            row_dot = jnp.sum(g.astype(F32) * context, axis=1, keepdims=True)
            grad_probs = dot(g, v[:keys], 1, 1)
            grad_scores = (probs * (grad_probs - row_dot)).astype(BF)
            gq = rotate(dot(grad_scores, k_scaled[:keys], 1, 0), at, -1.0)
            grad_out[0, at, cq] = gq.astype(BF)
            one = jnp.sum(gq, axis=0, keepdims=True)
            sum_q = one if sum_q is None else sum_q + one
            gk = dot(grad_scores, q[at], 0, 0)
            gv = dot(probs_b, g, 0, 0)
            if p == 0:
                acc_k[:keys], acc_v[:keys] = gk, gv
            else:
                acc_k[:part] += gk[:part]
                acc_v[:part] += gv[:part]
                acc_k[part:keys], acc_v[part:keys] = gk[part:], gv[part:]
        gk = rotate(acc_k[...], every, -1.0)
        gv = acc_v[...]
        grad_out[0, :, ck] = gk.astype(BF)
        grad_out[0, :, cv] = gv.astype(BF)
        sums[0, :, cq] = jnp.broadcast_to(sum_q, (8, HEAD))
        sums[0, :, ck] = jnp.broadcast_to(jnp.sum(gk, axis=0, keepdims=True), (8, HEAD))
        sums[0, :, cv] = jnp.broadcast_to(jnp.sum(gv, axis=0, keepdims=True), (8, HEAD))


def gelu_and_slope(a):
    half_erf = 0.5 * lax.erf(a * 0.7071067811865476)
    cdf = 0.5 + half_erf
    slope = cdf + a * (jnp.exp(-0.5 * a * a) * 0.3989422804014327)
    return a * cdf, slope


def step_kernel(nbits, names, *refs):
    r = dict(zip(names, refs, strict=True))
    hid, cot, tab, small = r["hid"], r["cot"], r["tab"], r["small"]
    wqkv, wdense, wfc1, wfc2 = r["wqkv"], r["wdense"], r["wfc1"], r["wfc2"]
    xall, call, tall = r["xall"], r["call"], r["tall"]
    n1, n2, st = r["n1"], r["n2"], r["st"]
    gctx, gact, act, gpre, fsum = r["gctx"], r["gact"], r["act"], r["gpre"], r["fsum"]
    ctx, gpk, qsum = r["ctx"], r["gpk"], r["qsum"]
    outp, outr, outx = r["outp"], r["outr"], r["outx"]
    up, ur, ux, usum = r["up"], r["ur"], r["ux"], r["usum"]
    wq, wf1, wf2, wd = r["wq"], r["wf1"], r["wf2"], r["wd"]
    sm_own, sm_got, sm = r["sm_own"], r["sm_got"], r["sm"]

    me = Place(nbits)
    s, c = me.s, me.c
    rows, width = hid.shape
    half = width // 2
    quarter = width // 4
    ffq = wf2.shape[0]
    mine = tuple(me.bits)
    every = (slice(None),) * (nbits + 1)
    mv = Mover(r["send"], r["recv"], r["lsem"])
    near, far = pl.ds(0, 2), pl.ds(2, 2)

    bring = [
        mv.local(small, sm_own),
        mv.local(wfc2.at[ds(c * ffq, ffq)], wf2),
        mv.local(wdense.at[ds(c * quarter, quarter)], wd),
    ]
    bring_w = [mv.local(wfc1.at[every + (ds((2 * s + c) * ffq, ffq),)], wf1.at[s])] + [
        mv.local(
            wqkv.at[every + (ds(g * width + (2 * s + c) * quarter, quarter),)],
            wq.at[(s,) + every + (pl.ds(g * quarter, quarter),)],
        )
        for g in range(3)
    ]
    me.barrier()

    away = 2 * (1 - s) + c
    x_small = mv.remote(small, sm_got, me.over_x)
    x_q = [
        mv.remote(
            wqkv.at[mine + (slice(None), ds(g * width + away * quarter, quarter))],
            wq.at[(s,) + mine + (slice(None), pl.ds(g * quarter, quarter))],
            me.over_x,
        )
        for g in range(3)
    ]
    x_f1 = mv.remote(
        wfc1.at[mine + (slice(None), ds(away * ffq, ffq))], wf1.at[(s,) + mine], me.over_x
    )
    x_hid = mv.remote(hid, xall.at[2], me.over_x)
    x_cot = mv.remote(cot, call.at[2], me.over_x)
    c_cot = mv.remote(cot, call.at[1], me.over_core)
    c_hid = mv.remote(hid, xall.at[1], me.over_core)
    c_tab = mv.remote(tab, tall.at[1], me.over_core)

    last_bit = nbits - 1

    class Spread:
        def __init__(self, w, first):
            self.w, self.flying, self.final, self.b = w, first, [], 0

        def go(self):
            arrived(self.flying)
            self.flying = []
            b = self.b
            if b < last_bit:
                at = tuple(slice(None) if k < b else me.bits[k] for k in range(nbits))
                self.flying.append(
                    mv.remote(self.w.at[(1 - s,) + at], self.w.at[(1 - s,) + at], me.over_bit(b))
                )
            at = tuple(
                slice(None) if k < b - 1 else (1 - me.bits[k] if k == b - 1 else me.bits[k])
                for k in range(nbits)
            )
            self.final.append(
                mv.remote(self.w.at[(1 - s,) + at], self.w.at[(1 - s,) + at], me.over_bit(last_bit))
            )
            self.b += 1

        def done(self):
            while self.b <= last_bit:
                self.go()
            arrived(self.final)

    acc, got = r["acc"], r["got"]
    acc[0] = jnp.zeros(acc.shape[1:], F32)

    def stage(own_x, own_c, own_t):
        pairs = ((hid, own_x, xall.at[0]), (cot, own_c, call.at[0]), (tab, own_t, tall.at[0]))
        for one in [mv.local(a, b) for a, b, _ in pairs]:
            one.wait()
        out = [mv.local(b, o) for _, b, o in pairs]
        acc[0, 4:5, :] = jnp.sum(own_c[...].astype(F32), axis=0, keepdims=True)
        for one in out:
            one.wait()

    pl.run_scoped(
        stage,
        pltpu.VMEM((rows, width), BF),
        pltpu.VMEM((rows, width), BF),
        pltpu.VMEM((rows, 128), F32),
    )
    for one in bring:
        one.wait()

    tile = min(512, ffq)
    sub = rows // 2
    tok2 = lambda i, j: (i, j, 0)

    def from_cot(at):
        def body(a, o, ob):
            for k in range(ffq // tile):
                cols = pl.ds(k * tile, tile)
                o[0, :, cols] = dot(a[0], wf2[cols, :], 1, 1)
            ob[0] = dot(a[0], wd[...], 1, 1).astype(BF)

        pipe(
            body,
            (2, 2),
            [(call.at[at], (1, sub, width), tok2)],
            [(gact.at[at], (1, sub, ffq), tok2), (gctx.at[at], (1, sub, quarter), tok2)],
        )

    def from_cot_after(at):
        def body(a, slope, o, ob, o_sum):
            for k in range(ffq // tile):
                cols = pl.ds(k * tile, tile)
                grad = dot(a[0], wf2[cols, :], 1, 1) * slope[0, :, cols]
                o[0, :, cols] = grad.astype(BF)
                o_sum[0, :, cols] = jnp.broadcast_to(
                    jnp.sum(grad, axis=0, keepdims=True), (8, tile)
                )
            ob[0] = dot(a[0], wd[...], 1, 1).astype(BF)

        pipe(
            body,
            (2, 2),
            [(call.at[at], (1, sub, width), tok2), (gact.at[at], (1, sub, ffq), tok2)],
            [
                (gpre.at[at], (1, sub, ffq), tok2),
                (gctx.at[at], (1, sub, quarter), tok2),
                (fsum.at[at], (1, 8, ffq), tok2),
            ],
        )

    def norm_blocks(at):
        def body(x, o1, o2, ost):
            o1[0], o2[0], ost[0] = normalize(x[0].astype(F32), sm, width)

        pipe(
            body,
            (2, 2),
            [(xall.at[at], (1, sub, width), tok2)],
            [
                (n1.at[at], (1, sub, width), tok2),
                (n2.at[at], (1, sub, width), tok2),
                (st.at[at], (1, sub, 128), tok2),
            ],
        )

    bias_q = lambda g: sm[:, ds(4 * width + g * width + (2 * s + c) * quarter, quarter)]
    bias_f = lambda k: sm[:, ds(7 * width + (2 * s + c) * ffq + k * tile, tile)]
    all_rows = (slice(None),) + every

    def hidden_units(at):
        def body(a, g, o_act, o_pre, o_sum):
            for k in range(ffq // tile):
                cols = pl.ds(k * tile, tile)
                pre = dot(a[0], flat(wf1[all_rows + (cols,)]), 1, 0) + bias_f(k)
                value, slope = gelu_and_slope(pre)
                o_act[0, :, cols] = value.astype(BF)
                grad = g[0, :, cols] * slope
                o_pre[0, :, cols] = grad.astype(BF)
                o_sum[0, :, cols] = jnp.broadcast_to(
                    jnp.sum(grad, axis=0, keepdims=True), (8, tile)
                )

        pipe(
            body,
            (2, 2),
            [(n2.at[at], (1, sub, width), tok2), (gact.at[at], (1, sub, ffq), tok2)],
            [
                (act.at[at], (1, sub, ffq), tok2),
                (gpre.at[at], (1, sub, ffq), tok2),
                (fsum.at[at], (1, 8, ffq), tok2),
            ],
        )

    def forward(at):
        def body(two, o_act, o_slope):
            for k in range(ffq // tile):
                cols = pl.ds(k * tile, tile)
                pre = dot(two[0], flat(wf1[all_rows + (cols,)]), 1, 0) + bias_f(k)
                value, slope = gelu_and_slope(pre)
                o_act[0, :, cols] = value.astype(BF)
                o_slope[0, :, cols] = slope

        pipe(
            body,
            (2, 2),
            [(n2.at[at], (1, sub, width), tok2)],
            [(act.at[at], (1, sub, ffq), tok2), (gact.at[at], (1, sub, ffq), tok2)],
        )

    def project(a, o):
        for g in range(3):
            cols = pl.ds(g * quarter, quarter)
            o[:, cols] = dot(a[0], flat(wq[all_rows + (cols,)]), 1, 0) + bias_q(g)

    def attend(at):
        whole = lambda i: (i, 0, 0)
        pipe(
            partial(attention_body, r["acc_k"], r["acc_v"], r["packed"], project),
            (2,),
            [
                (n1.at[at], (1, rows, width), whole),
                (gctx.at[at], (1, rows, quarter), whole),
                (tall.at[at], (1, rows, 128), whole),
            ],
            [
                (ctx.at[at], (1, rows, quarter), whole),
                (gpk.at[at], (1, rows, 3 * quarter), whole),
                (qsum.at[at], (1, 8, 3 * quarter), whole),
            ],
        )

    def finish(at, out=True, grad=True, plus=()):
        more = list(plus)

        def body(*refs):
            refs = list(refs)
            take = lambda n: [refs.pop(0) for _ in range(n)]
            if out:
                a, b = take(2)
            if grad:
                ga, gb, x, stat = take(4)
            extra = take(len(more))
            if out:
                o = refs.pop(0)
                for k in range(4):
                    cols = pl.ds(k * quarter, quarter)
                    value = dot(a[0], wd[:, cols], 1, 0) + dot(b[0], wf2[:, cols], 1, 0)
                    if more:
                        value = value + extra[0][0, :, cols].astype(F32)
                    o[0, :, cols] = value.astype(BF)
            if not grad:
                return
            ou, osum = refs
            mean, rstd = stat[0, :, 0:1], stat[0, :, 1:2]
            for k in range(4):
                cols = pl.ds(k * quarter, quarter)
                one = dot(ga[0], flat(wq[k // 2, k % 2]), 1, 1)
                two = dot(gb[0], flat(wf1[k // 2, k % 2]), 1, 1)
                n = (x[0, :, cols].astype(F32) - mean) * rstd
                value = (
                    one * sm[:, pl.ds(k * quarter, quarter)]
                    + two * sm[:, pl.ds(2 * width + k * quarter, quarter)]
                )
                if more:
                    value = value + extra[-1][0, :, cols].astype(F32)
                ou[0, :, cols] = value.astype(BF)
                osum[0, 0:1, cols] = jnp.sum(one * n, axis=0, keepdims=True)
                osum[0, 1:2, cols] = jnp.sum(one, axis=0, keepdims=True)
                osum[0, 2:3, cols] = jnp.sum(two * n, axis=0, keepdims=True)
                osum[0, 3:4, cols] = jnp.sum(two, axis=0, keepdims=True)

        ins, outs = [], []
        if out:
            ins += [(ctx.at[at], (1, sub, quarter), tok2), (act.at[at], (1, sub, ffq), tok2)]
            outs += [(outp.at[at], (1, sub, width), tok2)]
        if grad:
            ins += [
                (gpk.at[at], (1, sub, 3 * quarter), tok2),
                (gpre.at[at], (1, sub, ffq), tok2),
                (xall.at[at], (1, sub, width), tok2),
                (st.at[at], (1, sub, 128), tok2),
            ]
            outs += [(up.at[at], (1, sub, width), tok2), (usum.at[at], (1, 8, width), tok2)]
        ins += [(v, (1, sub, width), tok2) for v in more]
        pipe(body, (at.size, 2), ins, outs)

    def row_grad(lhs, keep, send, first, cols_tile, count):
        per_owner = keep.shape[-2]
        dims = keep.shape[:-2]
        lw = lhs.shape[2]

        def body(a, b, o_keep, o_send):
            full = dot(flat(a[...]), flat(b[...]), 0, 0).astype(BF)
            full = full.reshape((lw // (2 * per_owner), 2, per_owner, full.shape[-1]))
            zero, one = full[:, 0], full[:, 1]
            o_keep[...] = jnp.where(c == 0, zero, one).reshape(o_keep.shape)
            o_send[...] = jnp.where(c == 0, one, zero).reshape(o_send.shape)

        block = dims + (per_owner, cols_tile)
        at = lambda j: (0,) * (len(dims) + 1) + (j,)
        pipe(
            body,
            (count,),
            [
                (lhs, (4, rows, lw), lambda j: (0, 0, 0), True),
                (call, (4, rows, cols_tile), lambda j: (0, 0, first + j)),
            ],
            [(keep, block, at), (send, block, at)],
        )

    def column_grad(lhs, rhs, out, first, count):
        block = (1, 1) + out.shape[2:]

        def body(a, b, o):
            o[...] = dot(flat(a[...]), flat(b[...]), 0, 0).astype(BF).reshape(block)

        pipe(
            body,
            (count,),
            [
                (lhs, (4, rows, quarter), lambda j: (0, 0, first + j)),
                (rhs, (4, rows, rhs.shape[2]), lambda j: (0, 0, 0), True),
            ],
            [(out, block, lambda j: ((first + j) // 2, (first + j) % 2) + (0,) * (len(block) - 2))],
        )

    usual = tuple(reversed(range(nbits)))

    def order_of(name):
        return tuple("hly".index(one) for one in name) if nbits == 3 else usual

    def reduction(name, g, order, came):
        return Reduce(
            me,
            mv,
            g,
            order,
            [r[f"{name}_got{t}"] for t in range(nbits)],
            [r[f"{name}_sum{t}"] for t in range(1, nbits)],
            [r[f"{name}_ahead{t}"] for t in range(2, nbits + 1)],
            r[came],
        )

    f1 = Spread(wf1, [x_f1])
    q = Spread(wq, x_q)
    q.go()
    x_f1.wait_recv()
    f1.flying = []
    c_cot.wait_recv()
    from_cot(near)
    x_small.wait_recv()
    lo = 0
    for n in (half, half, half, half, 3 * half, ffq * 2, half, half):
        sm[:, ds(2 * lo + s * n, n, 128)] = sm_own[:, pl.ds(lo, n)]
        sm[:, ds(2 * lo + (1 - s) * n, n, 128)] = sm_got[:, pl.ds(lo, n)]
        lo += n
    arrived([c_hid, c_tab])
    norm_blocks(near)
    q.go()
    f1.go()
    for one in bring_w:
        one.wait()
    for _ in range(2, nbits):
        q.go()
        f1.go()
    x_hid.wait_recv()
    d_hid = mv.remote(xall.at[2], xall.at[3], me.over_core)
    while f1.b <= last_bit:
        f1.go()
    d_hid.wait_recv()
    norm_blocks(far)
    q.done()
    attend(near)
    f1.done()
    hidden_units(near)
    x_cot.wait_recv()
    d_cot = mv.remote(call.at[2], call.at[3], me.over_core)
    x_tab = mv.remote(tab, tall.at[2], me.over_x)
    forward(far)
    d_cot.wait_recv()

    f2a, f2b, f2a_s, f2b_s = r["f2a"], r["f2b"], r["f2a_send"], r["f2b_send"]
    g1, gq, d = r["g1"], r["gq"], r["d"]
    third, second = pl.ds(3, 1), pl.ds(2, 1)
    row_grad(act, f2b.at[c], f2b_s, width // 1024, 512, width // 1024)
    f2b_swap = mv.remote(f2b_s, f2b.at[c], me.over_core)
    x_tab.wait_recv()
    d_tab = mv.remote(tall.at[2], tall.at[3], me.over_core)
    from_cot_after(far)
    f2b_swap.wait_recv()
    red_f2b = reduction("f2b", f2b, order_of("lyh"), "came_f2")
    red_f2b.go()
    column_grad(n2, gpre, g1, 2, 2)
    red_f1b = reduction("f1b", g1.at[1], order_of("ylh"), "came_f1")
    red_f1b.go()
    column_grad(n2, gpre, g1, 0, 2)
    red_f1a = reduction("f1a", g1.at[0], order_of("lhy"), "came_f1")
    red_f1a.go()
    d_tab.wait_recv()
    attend(far)
    red_f1b.go()
    red_f2b.go()
    column_grad(n1, gpk, gq, 2, 2)
    red_qb = reduction("q_b", gq.at[1], order_of("yhl"), "came_q_")
    red_qb.go()
    red_f1a.go()
    column_grad(n1, gpk, gq, 0, 2)
    red_qa = reduction("q_a", gq.at[0], order_of("lyh"), "came_q_")
    red_qa.go()
    red_f2b.go()
    finish(third, grad=False)
    o_far = mv.remote(outp.at[3], outr.at[1], me.over_core)
    red_f1b.go()
    row_grad(ctx, d.at[c], r["d_send"], 0, 512, width // 512)
    d_swap = mv.remote(r["d_send"], d.at[c], me.over_core)
    o_far.wait_recv()
    finish(second, grad=False, plus=(outr.at[pl.ds(1, 1)],))
    o_x = mv.remote(outp.at[2], outx, me.over_x)
    d_swap.wait_recv()
    red_d = reduction("d", d, order_of("ylh"), "came_d")
    red_d.go()
    row_grad(act, f2a.at[c], f2a_s, 0, 512, width // 1024)
    f2a_swap = mv.remote(f2a_s, f2a.at[c], me.over_core)
    red_qb.go()
    red_f1a.go()
    f2a_swap.wait_recv()
    red_f2a = reduction("f2a", f2a, order_of("ylh"), "came_f2")
    red_f2a.go()
    finish(third, out=False)
    u_far = mv.remote(up.at[3], ur.at[1], me.over_core)
    red_d.go()
    u_far.wait_recv()
    finish(second, out=False, plus=(ur.at[pl.ds(1, 1)],))
    u_x = mv.remote(up.at[2], ux, me.over_x)
    red_qa.go()
    finish(near)
    u_near = mv.remote(up.at[1], ur.at[0], me.over_core)
    o_near = mv.remote(outp.at[1], outr.at[0], me.over_core)

    def add_small(usum_v, qsum_v, fsum_v):
        for one in [mv.local(usum, usum_v), mv.local(qsum, qsum_v), mv.local(fsum, fsum_v)]:
            one.wait()
        acc[0, 0:4, :] = jnp.sum(usum_v[:, 0:4, :] + usum_v[:, 8:12, :], axis=0)
        for g in range(3):
            acc[0, 5 + g : 6 + g, ds((2 * s + c) * quarter, quarter)] = jnp.sum(
                qsum_v[:, 0:1, pl.ds(g * quarter, quarter)], axis=0
            )
        f_row = jnp.sum(fsum_v[:, 0:1, :] + fsum_v[:, 8:9, :], axis=0)
        acc[0, 8:9, ds(c * ffq, ffq)] = jnp.where(s == 0, f_row, 0.0)
        acc[0, 9:10, ds(c * ffq, ffq)] = jnp.where(s == 0, 0.0, f_row)

    pl.run_scoped(
        add_small,
        pltpu.VMEM((4, 16, width), F32),
        pltpu.VMEM((4, 8, 3 * quarter), F32),
        pltpu.VMEM((4, 16, ffq), F32),
    )
    small_peers = [me.over_core] + [me.over_bit(b) for b in range(nbits)] + [me.over_x]
    small_step = [0, None]

    def small_go():
        k, flying = small_step
        if k > len(small_peers):
            return
        if flying is not None:
            flying.wait_recv()
            acc[k] = acc[k - 1] + got[k - 1]
        if k < len(small_peers):
            small_step[1] = mv.remote(acc.at[k], got.at[k], small_peers[k])
        else:
            r["tot"][...] = acc[k]
        small_step[0] = k + 1


    small_go()
    red_f2a.go()
    small_go()
    red_qa.go()
    red_qb.go()
    small_go()
    red_d.go()
    red_f2a.go()
    small_go()


    for _ in range(nbits):
        for one in (red_f2a, red_f2b, red_f1a, red_f1b, red_qa, red_d, red_qb):
            if one.step < nbits:
                one.go()
    tok = lambda i: (i, 0)
    block = (rows // 8, width)

    def result_body(x, y, a, b, e, ua, ub, ue, stat, o, ou):
        xf = x[...].astype(F32)
        o[...] = (
            xf
            + (
                a[...].astype(F32)
                + b[...].astype(F32)
                + e[...].astype(F32)
                + (sm[:, pl.ds(7 * width + 4 * ffq, width)] + sm[:, pl.ds(8 * width + 4 * ffq, width)])
            )
        ).astype(BF)
        u = ua[...].astype(F32) + ub[...].astype(F32) + ue[...].astype(F32)
        mean, rstd = stat[:, 0:1], stat[:, 1:2]
        n = (xf - mean) * rstd
        ou[...] = y[...].astype(F32) + rstd * (
            u - jnp.mean(u, axis=1, keepdims=True) - n * jnp.mean(u * n, axis=1, keepdims=True)
        )

    last = []

    def hand_over(e, got):
        last.append(mv.remote(e.at[s, 1 - c], got.at[0], me.over_core))
        last.append(mv.remote(e.at[1 - s, c], got.at[1], me.over_x))
        last.append(mv.remote(e.at[1 - s, 1 - c], got.at[2], me.diagonal))

    e_f1, e_q, r_f1, r_q = r["e_f1"], r["e_q"], r["r_f1"], r["r_q"]

    def owners(end_f, end_q, o_f1, o_q, o_f2, o_d):
        before = len(mv.sent)
        for k, red in enumerate((red_f1a, red_f1b)):
            red.end(end_f)
            e_f1[k] = end_f[...].reshape(e_f1.shape[1:])
        hand_over(e_f1, r_f1)
        for k, red in ((1, red_qb), (0, red_qa)):
            red.end(end_q)
            e_q[k] = end_q[...].reshape(e_q.shape[1:])
        hand_over(e_q, r_q)
        arrived([o_near, u_near, o_x, u_x])
        small_go()
        pipe(
            result_body,
            (8,),
            [
                (v, block, tok)
                for v in (hid, cot, outp.at[0], outr.at[0], outx, up.at[0], ur.at[0], ux)
            ]
            + [(st.at[0], (rows // 8, 128), tok)],
            [(r["result"], block, tok), (r["grad"], block, tok)],
        )
        places = ((s, c), (s, 1 - c), (1 - s, c), (1 - s, 1 - c))
        arrived(last)
        for k, (ps, pc) in enumerate(places):
            part = e_f1[s, c] if k == 0 else r_f1[k - 1]
            o_f1[:, ds((2 * ps + pc) * ffq, ffq)] = part.astype(F32)
        out = [mv.local(o_f1, r["o_f1"])]
        for k, (ps, pc) in enumerate(places):
            for g in range(3):
                cols = pl.ds(g * quarter, quarter)
                part = e_q[s, c, :, cols] if k == 0 else r_q[k - 1, :, cols]
                o_q[:, ds(g * width + (2 * ps + pc) * quarter, quarter)] = part.astype(F32)
        out.append(mv.local(o_q, r["o_q"]))
        for _ in range(nbits + 3):
            small_go()
        red_f2b.end(o_f2.at[:, pl.ds(half, half)])
        red_d.end(o_d)
        out.append(mv.local(o_d, r["o_d"]))
        red_f2a.end(o_f2.at[:, pl.ds(0, half)])
        out.append(mv.local(o_f2, r["o_f2"]))
        for one in out:
            one.wait()
        for one in mv.sent[before:]:
            one.wait_send()
        del mv.sent[before:]

    pl.run_scoped(
        owners,
        pltpu.VMEM(g1.shape[-2:], BF),
        pltpu.VMEM(gq.shape[-2:], BF),
        pltpu.VMEM(r["o_f1"].shape, F32),
        pltpu.VMEM(r["o_q"].shape, F32),
        pltpu.VMEM(r["o_f2"].shape, F32),
        pltpu.VMEM(r["o_d"].shape, F32),
    )
    mv.finish()


def step(nbits, hid, cot, tab, small, wqkv, wdense, wfc1, wfc2):
    rows, width = hid.shape
    half, ff = wfc1.shape
    quarter, ffq = width // 4, ff // 4
    groups = 2**nbits
    own_rows = half // groups
    half_own = own_rows // 2
    per_ff = ffq // groups
    length = small.shape[1]
    bits = (2,) * nbits
    hbm, vmem = pl.BlockSpec(memory_space=pl.ANY), pl.BlockSpec(memory_space=pltpu.VMEM)
    sds = jax.ShapeDtypeStruct
    outs = {
        "result": (hbm, (rows, width), BF),
        "grad": (hbm, (rows, width), F32),
        "o_f2": (hbm, (per_ff, width), F32),
        "o_d": (hbm, (half_own, width), F32),
        "o_f1": (hbm, (half_own, ff), F32),
        "o_q": (hbm, (half_own, 3 * width), F32),
        "tot": (vmem, (16, width), F32),
        "xall": (hbm, (4, rows, width), BF),
        "call": (hbm, (4, rows, width), BF),
        "tall": (hbm, (4, rows, 128), F32),
        "n1": (hbm, (4, rows, width), BF),
        "n2": (hbm, (4, rows, width), BF),
        "st": (hbm, (4, rows, 128), F32),
        "gctx": (hbm, (4, rows, quarter), BF),
        "gact": (hbm, (4, rows, ffq), F32),
        "act": (hbm, (4, rows, ffq), BF),
        "gpre": (hbm, (4, rows, ffq), BF),
        "fsum": (hbm, (4, 16, ffq), F32),
        "ctx": (hbm, (4, rows, quarter), BF),
        "gpk": (hbm, (4, rows, 3 * quarter), BF),
        "qsum": (hbm, (4, 8, 3 * quarter), F32),
        "f2a": (hbm, bits + (per_ff, half), BF),
        "f2b": (hbm, bits + (per_ff, half), BF),
        "f2a_send": (hbm, bits[1:] + (per_ff, half), BF),
        "f2b_send": (hbm, bits[1:] + (per_ff, half), BF),
        "g1": (hbm, (2,) + bits + (own_rows, ffq), BF),
        "d": (hbm, bits + (half_own, width), BF),
        "d_send": (hbm, bits[1:] + (half_own, width), BF),
        "gq": (hbm, (2,) + bits + (own_rows, 3 * quarter), BF),
        "outp": (hbm, (4, rows, width), BF),
        "outr": (hbm, (2, rows, width), BF),
        "outx": (hbm, (rows, width), BF),
        "up": (hbm, (4, rows, width), BF),
        "ur": (hbm, (2, rows, width), BF),
        "ux": (hbm, (rows, width), BF),
        "usum": (hbm, (4, 16, width), F32),
    }
    extra = {}
    for name, tail in (
        ("f2a", (per_ff, half)),
        ("f2b", (per_ff, half)),
        ("f1a", (own_rows, ffq)),
        ("f1b", (own_rows, ffq)),
        ("d", (half_own, width)),
        ("q_a", (own_rows, 3 * quarter)),
        ("q_b", (own_rows, 3 * quarter)),
    ):
        for t in range(nbits):
            dims = (2,) * (nbits - 1 - t) + tail
            if t == 0:
                outs[f"{name}_got{t}"] = (hbm, dims, BF)
            else:
                extra[f"{name}_got{t}"] = pltpu.VMEM(dims, BF)
            if t == 1:
                extra[f"came_{name[:2]}"] = pltpu.VMEM(dims, BF)
            if t > 0:
                extra[f"{name}_sum{t}"] = pltpu.VMEM(dims, BF)
        for t in range(2, nbits + 1):
            dims = (2,) * max(nbits - 1 - t, 0) + tail
            extra[f"{name}_ahead{t}"] = pltpu.VMEM((2,) + dims, BF)
    scratch = {
        "wq": pltpu.VMEM((2,) + bits + (own_rows, 3 * quarter), BF),
        "wf1": pltpu.VMEM((2,) + bits + (own_rows, ffq), BF),
        "wf2": pltpu.VMEM((ffq, width), BF),
        "wd": pltpu.VMEM((quarter, width), BF),
        "sm_own": pltpu.VMEM((1, length), F32),
        "sm_got": pltpu.VMEM((1, length), F32),
        "sm": pltpu.VMEM((1, 2 * length), F32),
        "packed": pltpu.VMEM((rows, 3 * quarter), F32),
        "acc_k": pltpu.VMEM((rows, HEAD), F32),
        "acc_v": pltpu.VMEM((rows, HEAD), F32),
        "acc": pltpu.VMEM((3 + nbits, 16, width), F32),
        "got": pltpu.VMEM((2 + nbits, 16, width), F32),
        "r_f1": pltpu.VMEM((3, half_own, ffq), BF),
        "r_q": pltpu.VMEM((3, half_own, 3 * quarter), BF),
        "e_f1": pltpu.VMEM((2, 2, half_own, ffq), BF),
        "e_q": pltpu.VMEM((2, 2, half_own, 3 * quarter), BF),
        "send": pltpu.SemaphoreType.DMA((36 + 12 * nbits,)),
        "recv": pltpu.SemaphoreType.DMA((36 + 12 * nbits,)),
        "lsem": pltpu.SemaphoreType.DMA((40 + 14 * nbits,)),
        **extra,
    }
    ins = ("hid", "cot", "tab", "small", "wqkv", "wdense", "wfc1", "wfc2")
    got = pl.pallas_call(
        partial(step_kernel, nbits, ins + tuple(outs) + tuple(scratch)),
        in_specs=[hbm] * len(ins),
        out_specs=[one[0] for one in outs.values()],
        out_shape=[sds(*one[1:]) for one in outs.values()],
        scratch_shapes=list(scratch.values()),
        compiler_params=pltpu.CompilerParams(
            collective_id=0, has_side_effects=True, vmem_limit_bytes=VMEM_LIMIT
        ),
        name="step",
    )(
        hid,
        cot,
        tab,
        small,
        wqkv.reshape(bits + (own_rows, 3 * width)),
        wdense,
        wfc1.reshape(bits + (own_rows, ff)),
        wfc2,
    )
    return got[:7]


def rotary_table(seg):
    rows = seg.shape[0]
    index = jnp.arange(rows, dtype=jnp.int32)
    same = seg[:, None] == seg[None, :]
    first = jnp.min(jnp.where(same, index[None, :], rows), axis=1)
    offset = (index - first).astype(F32)
    frequency = jnp.exp(-jnp.log(10000.0) * jnp.arange(0, ROT, 2).astype(F32) / ROT)
    angles = offset[:, None] * frequency[None, :]
    ids = jnp.broadcast_to(seg.astype(F32)[:, None], (rows, 128 - ROT))
    return jnp.concatenate([jnp.cos(angles), jnp.sin(angles), ids], axis=1)


def local(
    nbits,
    hidden_in,
    out_cotangent,
    segment_ids,
    ln1_gain,
    ln1_bias,
    qkv_weight,
    qkv_bias,
    dense_weight,
    dense_bias,
    ln2_gain,
    ln2_bias,
    fc1_weight,
    fc1_bias,
    fc2_weight,
    fc2_bias,
):
    me = lax.axis_index("shard") * 2 ** (nbits + 1) + lax.axis_index("replica")
    owners = 2 ** (nbits + 2)
    width = hidden_in.shape[1]
    vectors = (
        ln1_gain, ln1_bias, ln2_gain, ln2_bias, qkv_bias, fc1_bias, dense_bias, fc2_bias
    )
    length = sum(v.shape[0] for v in vectors)
    small, lo = 0.0, 0
    for v in vectors:
        n = v.shape[0]
        small = small + jnp.pad(v.astype(F32), (lo, length - lo - n))
        lo += n
    result, grad, o_f2, o_d, o_f1, o_q, tot = step(
        nbits,
        hidden_in,
        out_cotangent,
        rotary_table(segment_ids),
        small[None],
        qkv_weight,
        dense_weight,
        fc1_weight,
        fc2_weight,
    )

    def own(v):
        return lax.dynamic_index_in_dim(v.reshape(v.shape[:-1] + (owners, -1)), me, v.ndim - 1, False)

    five = own(tot[:5])
    b_qkv = own(tot[5:8].reshape(-1))
    b_fc1 = own(tot[8:10].reshape(-1))
    return (
        result, grad, five[0], five[1], o_q, b_qkv, o_d, five[4],
        five[2], five[3], o_f1, b_fc1, o_f2, five[4],
    )


def solution(mesh):
    both = ("shard", "replica")
    nbits = (mesh.shape["replica"] // 2).bit_length() - 1
    wide, token, vector, matrix = P(both, None), P(both), P("shard"), P("shard", None)
    return jax.shard_map(
        partial(local, nbits),
        mesh=mesh,
        in_specs=(wide, wide, token, vector, vector, matrix, vector, matrix, vector)
        + (vector, vector, matrix, vector, matrix, vector),
        out_specs=(wide, wide, token, token, wide, token, wide, token)
        + (token, token, wide, token, wide, token),
        check_vma=False,
    )
```

```python
from functools import partial

import jax
import jax.numpy as jnp
from jax import lax
from jax.experimental import pallas as pl
from jax.experimental.pallas import tpu as pltpu
from jax.sharding import PartitionSpec as P

HEADS = 8
HEAD = 256
ROT = 64
NEG_FILL = -1e30
EPSILON = 1e-05
BF = jnp.bfloat16
F32 = jnp.float32
MESH = pl.DeviceIdType.MESH
ANY = pl.BlockSpec(memory_space=pl.ANY)
VMEM_LIMIT = 127 << 19


def dot(a, b, da, db):
    return lax.dot_general(a, b, (((da,), (db,)), ((), ())), preferred_element_type=F32)


def flat(v):
    return v.reshape((-1, v.shape[-1]))


class Place:
    def __init__(self, nbits):
        self.nbits = nbits
        self.s = lax.axis_index("shard")
        self.rep = lax.axis_index("replica")
        self.c = self.rep % 2
        self.r = self.rep // 2
        self.bits = [(self.r // 2 ** (nbits - 1 - b)) % 2 for b in range(nbits)]
        self.over_x = (1 - self.s, self.rep)
        self.over_core = (self.s, self.rep + 1 - 2 * self.c)
        self.diagonal = (1 - self.s, self.rep + 1 - 2 * self.c)

    def over_bit(self, b):
        return (self.s, self.rep + (1 - 2 * self.bits[b]) * 2 ** (self.nbits - b))

    def peers(self):
        return [self.over_x, self.over_core, self.diagonal] + [
            self.over_bit(b) for b in range(self.nbits)
        ]

    def barrier(self):
        sem = pltpu.get_barrier_semaphore()
        for peer in self.peers():
            pl.semaphore_signal(sem, inc=1, device_id=peer, device_id_type=MESH)
        pl.semaphore_wait(sem, 3 + self.nbits)


class Mover:
    def __init__(self, send, recv, local):
        self.send, self.recv, self.local_sems = send, recv, local
        self.n = self.m = 0
        self.sent = []

    def remote(self, src, dst, peer):
        one = pltpu.make_async_remote_copy(
            src_ref=src,
            dst_ref=dst,
            send_sem=self.send.at[self.n],
            recv_sem=self.recv.at[self.n],
            device_id=peer,
            device_id_type=MESH,
        )
        self.n += 1
        one.start()
        self.sent.append(one)
        return one

    def local(self, src, dst):
        one = pltpu.make_async_copy(src, dst, self.local_sems.at[self.m])
        self.m += 1
        one.start()
        return one

    def finish(self):
        for one in self.sent:
            one.wait_send()


def arrived(copies):
    for one in copies:
        one.wait_recv()


def pipe(body, grid, ins, outs):
    pltpu.emit_pipeline(
        body,
        grid=grid,
        in_specs=[
            pl.BlockSpec(v[1], v[2], pipeline_mode=pl.Buffered(1 if len(v) > 3 else 2)) for v in ins
        ],
        out_specs=[pl.BlockSpec(b, m) for _, b, m in outs],
    )(*[v[0] for v in ins], *[r for r, _, _ in outs])


def ds(start, size, step=None):
    return pl.ds(pl.multiple_of(start, step or size), size)


def normalize(x, sm, width):
    mean = jnp.mean(x, axis=1, keepdims=True)
    center = x - mean
    spread = jnp.mean(center * center, axis=1, keepdims=True)
    rstd = lax.rsqrt(spread + EPSILON)
    n = center * rstd
    one = (n * sm[:, pl.ds(0, width)] + sm[:, pl.ds(width, width)]).astype(BF)
    two = (n * sm[:, pl.ds(2 * width, width)] + sm[:, pl.ds(3 * width, width)]).astype(BF)
    lane = lax.broadcasted_iota(jnp.int32, (x.shape[0], 128), 1)
    return one, two, jnp.where(lane == 0, mean, rstd)


def blocks_of(shape):
    lead = len(shape) - 2
    return [tuple((m // 2 ** (lead - 1 - i)) % 2 for i in range(lead)) for m in range(2**lead)]


class Reduce:
    def __init__(self, me, mv, g, order, got, sums, ahead, came):
        self.me, self.mv, self.g, self.order = me, mv, g, order
        self.got, self.sums, self.ahead, self.came = got, sums, ahead, came
        self.step = 0
        self.flying = None
        self.fetched = []

    def at(self, level, step, last):
        gone = self.order[:level]
        out = []
        for b in range(self.me.nbits):
            if b in gone:
                continue
            if b in self.order[:step]:
                out.append(self.me.bits[b])
            elif step < len(self.order) and b == self.order[step]:
                out.append(last)
            else:
                out.append(slice(None))
        return tuple(out)

    def go(self):
        k = self.step
        if self.flying is not None:
            self.flying.wait_recv()
        b = self.order[k]
        other = 1 - self.me.bits[b]
        if k == 0:
            src = self.g.at[self.at(0, 0, other)]
            if self.me.nbits > 1:
                last = 1 - self.me.bits[self.order[1]]
                self.first = self.mv.local(self.g.at[self.at(0, 1, last)], self.sums[0])
        elif k == 1:
            src = self.sums[0]
            came = self.mv.local(self.got[0].at[self.at(1, 1, other)], self.came)
            for t in range(2, self.me.nbits + 1):
                last = 1 - self.me.bits[self.order[t]] if t < self.me.nbits else None
                for level, ref in ((0, self.g), (1, self.got[0])):
                    self.fetched.append(
                        self.mv.local(ref.at[self.at(level, t, last)], self.ahead[t - 2].at[level])
                    )
            self.first.wait()
            came.wait()
            for at in blocks_of(src.shape):
                src[at] = (src[at].astype(F32) + self.came[at].astype(F32)).astype(src.dtype)
        else:
            src = self.sums[k - 1]
            self.total(k, other, src)
        self.flying = self.mv.remote(src, self.got[k], self.me.over_bit(b))
        self.step += 1

    def total(self, k, last, out):
        for one in self.fetched[2 * (k - 2) : 2 * (k - 1)]:
            one.wait()
        near = self.ahead[k - 2]
        later = [self.got[j - 1].at[self.at(j, k, last)] for j in range(2, k + 1)]
        for at in blocks_of(out.shape):
            value = near[(0,) + at].astype(F32) + near[(1,) + at].astype(F32)
            for one in later:
                value = value + one[at].astype(F32)
            out[at] = value.astype(out.dtype)

    def end(self, out):
        self.flying.wait_recv()
        self.total(self.me.nbits, None, out)


def attention_body(acc_k, acc_v, packed, project, normed, gctx, tab, ctx_out, grad_out, sums):
    project(normed, packed)
    rows, width = gctx.shape[1:]
    t = tab[0]
    lane = lax.broadcasted_iota(jnp.int32, (rows, 128), 1)
    quart = ROT // 2
    cos = jnp.where(lane < quart, t, jnp.where(lane < ROT, pltpu.roll(t, quart, 1), 1.0))
    sin = jnp.where(lane < quart, -pltpu.roll(t, 128 - quart, 1), jnp.where(lane < ROT, t, 0.0))

    def rotate(v, at, sign):
        low = v[:, :128]
        swapped = jnp.where(
            lane[at] < quart, pltpu.roll(low, 128 - quart, 1), pltpu.roll(low, quart, 1)
        )
        return jnp.concatenate([low * cos[at] + swapped * (sign * sin[at]), v[:, 128:]], axis=1)

    ids_row = t.T[ROT : ROT + 1, :]
    inv_root = HEAD ** (-0.5)
    part = rows // 2
    every = slice(None)
    allowed = []
    for p in range(2):
        keys = (p + 1) * part
        row = p * part + lax.broadcasted_iota(jnp.int32, (part, keys), 0)
        col = lax.broadcasted_iota(jnp.int32, (part, keys), 1)
        same = t[p * part : (p + 1) * part, ROT : ROT + 1] == ids_row[:, :keys]
        allowed.append(same & (col <= row))
    for h in range(width // HEAD):
        cq = pl.ds(h * HEAD, HEAD)
        ck = pl.ds(width + h * HEAD, HEAD)
        cv = pl.ds(2 * width + h * HEAD, HEAD)
        q = (rotate(packed[:, cq], every, 1.0) * inv_root).astype(BF)
        k = rotate(packed[:, ck], every, 1.0).astype(BF)
        k_scaled = (k.astype(F32) * inv_root).astype(BF)
        v = packed[:, cv].astype(BF)
        sum_q = None
        for p in range(2):
            at = slice(p * part, (p + 1) * part)
            keys = (p + 1) * part
            g = gctx[0, at, cq]
            scores = jnp.where(allowed[p], dot(q[at], k[:keys], 1, 1), NEG_FILL)
            peak = jnp.max(scores, axis=1, keepdims=True)
            e = jnp.exp(scores - peak)
            total = jnp.sum(e, axis=1, keepdims=True)
            probs = e * (1.0 / total)
            probs_b = probs.astype(BF)
            context = dot(probs_b, v[:keys], 1, 0)
            ctx_out[0, at, cq] = context.astype(BF)
            row_dot = jnp.sum(g.astype(F32) * context, axis=1, keepdims=True)
            grad_probs = dot(g, v[:keys], 1, 1)
            grad_scores = (probs * (grad_probs - row_dot)).astype(BF)
            gq = rotate(dot(grad_scores, k_scaled[:keys], 1, 0), at, -1.0)
            grad_out[0, at, cq] = gq.astype(BF)
            one = jnp.sum(gq, axis=0, keepdims=True)
            sum_q = one if sum_q is None else sum_q + one
            gk = dot(grad_scores, q[at], 0, 0)
            gv = dot(probs_b, g, 0, 0)
            if p == 0:
                acc_k[:keys], acc_v[:keys] = gk, gv
            else:
                acc_k[:part] += gk[:part]
                acc_v[:part] += gv[:part]
                acc_k[part:keys], acc_v[part:keys] = gk[part:], gv[part:]
        gk = rotate(acc_k[...], every, -1.0)
        gv = acc_v[...]
        grad_out[0, :, ck] = gk.astype(BF)
        grad_out[0, :, cv] = gv.astype(BF)
        sums[0, :, cq] = jnp.broadcast_to(sum_q, (8, HEAD))
        sums[0, :, ck] = jnp.broadcast_to(jnp.sum(gk, axis=0, keepdims=True), (8, HEAD))
        sums[0, :, cv] = jnp.broadcast_to(jnp.sum(gv, axis=0, keepdims=True), (8, HEAD))


def gelu_and_slope(a):
    half_erf = 0.5 * lax.erf(a * 0.7071067811865476)
    cdf = 0.5 + half_erf
    slope = cdf + a * (jnp.exp(-0.5 * a * a) * 0.3989422804014327)
    return a * cdf, slope


def step_kernel(nbits, names, *refs):
    r = dict(zip(names, refs, strict=True))
    hid, cot, tab, small = r["hid"], r["cot"], r["tab"], r["small"]
    wqkv, wdense, wfc1, wfc2 = r["wqkv"], r["wdense"], r["wfc1"], r["wfc2"]
    xall, call, tall = r["xall"], r["call"], r["tall"]
    n1, n2, st = r["n1"], r["n2"], r["st"]
    gctx, gact, act, gpre, fsum = r["gctx"], r["gact"], r["act"], r["gpre"], r["fsum"]
    ctx, gpk, qsum = r["ctx"], r["gpk"], r["qsum"]
    outp, outr, outx = r["outp"], r["outr"], r["outx"]
    up, ur, ux, usum = r["up"], r["ur"], r["ux"], r["usum"]
    wq, wf1, wf2, wd = r["wq"], r["wf1"], r["wf2"], r["wd"]
    sm_own, sm_got, sm = r["sm_own"], r["sm_got"], r["sm"]

    me = Place(nbits)
    s, c = me.s, me.c
    rows, width = hid.shape
    half = width // 2
    quarter = width // 4
    ffq = wf2.shape[0]
    mine = tuple(me.bits)
    every = (slice(None),) * (nbits + 1)
    mv = Mover(r["send"], r["recv"], r["lsem"])
    near, far = pl.ds(0, 2), pl.ds(2, 2)

    bring = [
        mv.local(small, sm_own),
        mv.local(wfc2.at[ds(c * ffq, ffq)], wf2),
        mv.local(wdense.at[ds(c * quarter, quarter)], wd),
    ]
    bring_w = [mv.local(wfc1.at[every + (ds((2 * s + c) * ffq, ffq),)], wf1.at[s])] + [
        mv.local(
            wqkv.at[every + (ds(g * width + (2 * s + c) * quarter, quarter),)],
            wq.at[(s,) + every + (pl.ds(g * quarter, quarter),)],
        )
        for g in range(3)
    ]
    me.barrier()

    away = 2 * (1 - s) + c
    x_small = mv.remote(small, sm_got, me.over_x)
    x_q = [
        mv.remote(
            wqkv.at[mine + (slice(None), ds(g * width + away * quarter, quarter))],
            wq.at[(s,) + mine + (slice(None), pl.ds(g * quarter, quarter))],
            me.over_x,
        )
        for g in range(3)
    ]
    x_f1 = mv.remote(
        wfc1.at[mine + (slice(None), ds(away * ffq, ffq))], wf1.at[(s,) + mine], me.over_x
    )
    x_hid = mv.remote(hid, xall.at[2], me.over_x)
    x_cot = mv.remote(cot, call.at[2], me.over_x)
    c_cot = mv.remote(cot, call.at[1], me.over_core)
    c_hid = mv.remote(hid, xall.at[1], me.over_core)
    c_tab = mv.remote(tab, tall.at[1], me.over_core)

    last_bit = nbits - 1

    class Spread:
        def __init__(self, w, first):
            self.w, self.flying, self.final, self.b = w, first, [], 0

        def go(self):
            arrived(self.flying)
            self.flying = []
            b = self.b
            if b < last_bit:
                at = tuple(slice(None) if k < b else me.bits[k] for k in range(nbits))
                self.flying.append(
                    mv.remote(self.w.at[(1 - s,) + at], self.w.at[(1 - s,) + at], me.over_bit(b))
                )
            at = tuple(
                slice(None) if k < b - 1 else (1 - me.bits[k] if k == b - 1 else me.bits[k])
                for k in range(nbits)
            )
            self.final.append(
                mv.remote(self.w.at[(1 - s,) + at], self.w.at[(1 - s,) + at], me.over_bit(last_bit))
            )
            self.b += 1

        def done(self):
            while self.b <= last_bit:
                self.go()
            arrived(self.final)

    acc, got = r["acc"], r["got"]
    acc[0] = jnp.zeros(acc.shape[1:], F32)

    def stage(own_x, own_c, own_t):
        pairs = ((hid, own_x, xall.at[0]), (cot, own_c, call.at[0]), (tab, own_t, tall.at[0]))
        for one in [mv.local(a, b) for a, b, _ in pairs]:
            one.wait()
        out = [mv.local(b, o) for _, b, o in pairs]
        acc[0, 4:5, :] = jnp.sum(own_c[...].astype(F32), axis=0, keepdims=True)
        for one in out:
            one.wait()

    pl.run_scoped(
        stage,
        pltpu.VMEM((rows, width), BF),
        pltpu.VMEM((rows, width), BF),
        pltpu.VMEM((rows, 128), F32),
    )
    for one in bring:
        one.wait()

    tile = min(512, ffq)
    sub = rows // 2
    tok2 = lambda i, j: (i, j, 0)

    def from_cot(at):
        def body(a, o, ob):
            for k in range(ffq // tile):
                cols = pl.ds(k * tile, tile)
                o[0, :, cols] = dot(a[0], wf2[cols, :], 1, 1)
            ob[0] = dot(a[0], wd[...], 1, 1).astype(BF)

        pipe(
            body,
            (2, 2),
            [(call.at[at], (1, sub, width), tok2)],
            [(gact.at[at], (1, sub, ffq), tok2), (gctx.at[at], (1, sub, quarter), tok2)],
        )

    def from_cot_after(at):
        def body(a, slope, o, ob, o_sum):
            for k in range(ffq // tile):
                cols = pl.ds(k * tile, tile)
                grad = dot(a[0], wf2[cols, :], 1, 1) * slope[0, :, cols]
                o[0, :, cols] = grad.astype(BF)
                o_sum[0, :, cols] = jnp.broadcast_to(
                    jnp.sum(grad, axis=0, keepdims=True), (8, tile)
                )
            ob[0] = dot(a[0], wd[...], 1, 1).astype(BF)

        pipe(
            body,
            (2, 2),
            [(call.at[at], (1, sub, width), tok2), (gact.at[at], (1, sub, ffq), tok2)],
            [
                (gpre.at[at], (1, sub, ffq), tok2),
                (gctx.at[at], (1, sub, quarter), tok2),
                (fsum.at[at], (1, 8, ffq), tok2),
            ],
        )

    def norm_blocks(at):
        def body(x, o1, o2, ost):
            o1[0], o2[0], ost[0] = normalize(x[0].astype(F32), sm, width)

        pipe(
            body,
            (2, 2),
            [(xall.at[at], (1, sub, width), tok2)],
            [
                (n1.at[at], (1, sub, width), tok2),
                (n2.at[at], (1, sub, width), tok2),
                (st.at[at], (1, sub, 128), tok2),
            ],
        )

    bias_q = lambda g: sm[:, ds(4 * width + g * width + (2 * s + c) * quarter, quarter)]
    bias_f = lambda k: sm[:, ds(7 * width + (2 * s + c) * ffq + k * tile, tile)]
    all_rows = (slice(None),) + every

    def hidden_units(at):
        def body(a, g, o_act, o_pre, o_sum):
            for k in range(ffq // tile):
                cols = pl.ds(k * tile, tile)
                pre = dot(a[0], flat(wf1[all_rows + (cols,)]), 1, 0) + bias_f(k)
                value, slope = gelu_and_slope(pre)
                o_act[0, :, cols] = value.astype(BF)
                grad = g[0, :, cols] * slope
                o_pre[0, :, cols] = grad.astype(BF)
                o_sum[0, :, cols] = jnp.broadcast_to(
                    jnp.sum(grad, axis=0, keepdims=True), (8, tile)
                )

        pipe(
            body,
            (2, 2),
            [(n2.at[at], (1, sub, width), tok2), (gact.at[at], (1, sub, ffq), tok2)],
            [
                (act.at[at], (1, sub, ffq), tok2),
                (gpre.at[at], (1, sub, ffq), tok2),
                (fsum.at[at], (1, 8, ffq), tok2),
            ],
        )

    def forward(at):
        def body(two, o_act, o_slope):
            for k in range(ffq // tile):
                cols = pl.ds(k * tile, tile)
                pre = dot(two[0], flat(wf1[all_rows + (cols,)]), 1, 0) + bias_f(k)
                value, slope = gelu_and_slope(pre)
                o_act[0, :, cols] = value.astype(BF)
                o_slope[0, :, cols] = slope

        pipe(
            body,
            (2, 2),
            [(n2.at[at], (1, sub, width), tok2)],
            [(act.at[at], (1, sub, ffq), tok2), (gact.at[at], (1, sub, ffq), tok2)],
        )

    def project(a, o):
        for g in range(3):
            cols = pl.ds(g * quarter, quarter)
            o[:, cols] = dot(a[0], flat(wq[all_rows + (cols,)]), 1, 0) + bias_q(g)

    def attend(at):
        whole = lambda i: (i, 0, 0)
        pipe(
            partial(attention_body, r["acc_k"], r["acc_v"], r["packed"], project),
            (2,),
            [
                (n1.at[at], (1, rows, width), whole),
                (gctx.at[at], (1, rows, quarter), whole),
                (tall.at[at], (1, rows, 128), whole),
            ],
            [
                (ctx.at[at], (1, rows, quarter), whole),
                (gpk.at[at], (1, rows, 3 * quarter), whole),
                (qsum.at[at], (1, 8, 3 * quarter), whole),
            ],
        )

    def finish(at, out=True, grad=True, plus=()):
        more = list(plus)

        def body(*refs):
            refs = list(refs)
            take = lambda n: [refs.pop(0) for _ in range(n)]
            if out:
                a, b = take(2)
            if grad:
                ga, gb, x, stat = take(4)
            extra = take(len(more))
            if out:
                o = refs.pop(0)
                for k in range(4):
                    cols = pl.ds(k * quarter, quarter)
                    value = dot(a[0], wd[:, cols], 1, 0) + dot(b[0], wf2[:, cols], 1, 0)
                    if more:
                        value = value + extra[0][0, :, cols].astype(F32)
                    o[0, :, cols] = value.astype(BF)
            if not grad:
                return
            ou, osum = refs
            mean, rstd = stat[0, :, 0:1], stat[0, :, 1:2]
            for k in range(4):
                cols = pl.ds(k * quarter, quarter)
                one = dot(ga[0], flat(wq[k // 2, k % 2]), 1, 1)
                two = dot(gb[0], flat(wf1[k // 2, k % 2]), 1, 1)
                n = (x[0, :, cols].astype(F32) - mean) * rstd
                value = (
                    one * sm[:, pl.ds(k * quarter, quarter)]
                    + two * sm[:, pl.ds(2 * width + k * quarter, quarter)]
                )
                if more:
                    value = value + extra[-1][0, :, cols].astype(F32)
                ou[0, :, cols] = value.astype(BF)
                osum[0, 0:1, cols] = jnp.sum(one * n, axis=0, keepdims=True)
                osum[0, 1:2, cols] = jnp.sum(one, axis=0, keepdims=True)
                osum[0, 2:3, cols] = jnp.sum(two * n, axis=0, keepdims=True)
                osum[0, 3:4, cols] = jnp.sum(two, axis=0, keepdims=True)

        ins, outs = [], []
        if out:
            ins += [(ctx.at[at], (1, sub, quarter), tok2), (act.at[at], (1, sub, ffq), tok2)]
            outs += [(outp.at[at], (1, sub, width), tok2)]
        if grad:
            ins += [
                (gpk.at[at], (1, sub, 3 * quarter), tok2),
                (gpre.at[at], (1, sub, ffq), tok2),
                (xall.at[at], (1, sub, width), tok2),
                (st.at[at], (1, sub, 128), tok2),
            ]
            outs += [(up.at[at], (1, sub, width), tok2), (usum.at[at], (1, 8, width), tok2)]
        ins += [(v, (1, sub, width), tok2) for v in more]
        pipe(body, (at.size, 2), ins, outs)

    def row_grad(lhs, keep, send, first, cols_tile, count):
        per_owner = keep.shape[-2]
        dims = keep.shape[:-2]
        lw = lhs.shape[2]

        def body(a, b, o_keep, o_send):
            full = dot(flat(a[...]), flat(b[...]), 0, 0).astype(BF)
            full = full.reshape((lw // (2 * per_owner), 2, per_owner, full.shape[-1]))
            zero, one = full[:, 0], full[:, 1]
            o_keep[...] = jnp.where(c == 0, zero, one).reshape(o_keep.shape)
            o_send[...] = jnp.where(c == 0, one, zero).reshape(o_send.shape)

        block = dims + (per_owner, cols_tile)
        at = lambda j: (0,) * (len(dims) + 1) + (j,)
        pipe(
            body,
            (count,),
            [
                (lhs, (4, rows, lw), lambda j: (0, 0, 0), True),
                (call, (4, rows, cols_tile), lambda j: (0, 0, first + j)),
            ],
            [(keep, block, at), (send, block, at)],
        )

    def column_grad(lhs, rhs, out, first, count):
        block = (1, 1) + out.shape[2:]

        def body(a, b, o):
            o[...] = dot(flat(a[...]), flat(b[...]), 0, 0).astype(BF).reshape(block)

        pipe(
            body,
            (count,),
            [
                (lhs, (4, rows, quarter), lambda j: (0, 0, first + j)),
                (rhs, (4, rows, rhs.shape[2]), lambda j: (0, 0, 0), True),
            ],
            [(out, block, lambda j: ((first + j) // 2, (first + j) % 2) + (0,) * (len(block) - 2))],
        )

    usual = tuple(reversed(range(nbits)))

    def order_of(name):
        return tuple("hly".index(one) for one in name) if nbits == 3 else usual

    def reduction(name, g, order, came):
        return Reduce(
            me,
            mv,
            g,
            order,
            [r[f"{name}_got{t}"] for t in range(nbits)],
            [r[f"{name}_sum{t}"] for t in range(1, nbits)],
            [r[f"{name}_ahead{t}"] for t in range(2, nbits + 1)],
            r[came],
        )

    f1 = Spread(wf1, [x_f1])
    q = Spread(wq, x_q)
    q.go()
    x_f1.wait_recv()
    f1.flying = []
    c_cot.wait_recv()
    from_cot(near)
    x_small.wait_recv()
    lo = 0
    for n in (half, half, half, half, 3 * half, ffq * 2, half, half):
        sm[:, ds(2 * lo + s * n, n, 128)] = sm_own[:, pl.ds(lo, n)]
        sm[:, ds(2 * lo + (1 - s) * n, n, 128)] = sm_got[:, pl.ds(lo, n)]
        lo += n
    arrived([c_hid, c_tab])
    norm_blocks(near)
    q.go()
    f1.go()
    for one in bring_w:
        one.wait()
    for _ in range(2, nbits):
        q.go()
        f1.go()
    x_hid.wait_recv()
    d_hid = mv.remote(xall.at[2], xall.at[3], me.over_core)
    while f1.b <= last_bit:
        f1.go()
    d_hid.wait_recv()
    norm_blocks(far)
    q.done()
    attend(near)
    f1.done()
    hidden_units(near)
    x_cot.wait_recv()
    d_cot = mv.remote(call.at[2], call.at[3], me.over_core)
    x_tab = mv.remote(tab, tall.at[2], me.over_x)
    forward(far)
    d_cot.wait_recv()

    f2a, f2b, f2a_s, f2b_s = r["f2a"], r["f2b"], r["f2a_send"], r["f2b_send"]
    g1, gq, d = r["g1"], r["gq"], r["d"]
    third, second = pl.ds(3, 1), pl.ds(2, 1)
    row_grad(act, f2b.at[c], f2b_s, width // 1024, 512, width // 1024)
    f2b_swap = mv.remote(f2b_s, f2b.at[c], me.over_core)
    x_tab.wait_recv()
    d_tab = mv.remote(tall.at[2], tall.at[3], me.over_core)
    from_cot_after(far)
    f2b_swap.wait_recv()
    red_f2b = reduction("f2b", f2b, order_of("lyh"), "came_f2")
    red_f2b.go()
    column_grad(n2, gpre, g1, 2, 2)
    red_f1b = reduction("f1b", g1.at[1], order_of("ylh"), "came_f1")
    red_f1b.go()
    column_grad(n2, gpre, g1, 0, 2)
    red_f1a = reduction("f1a", g1.at[0], order_of("lhy"), "came_f1")
    red_f1a.go()
    d_tab.wait_recv()
    attend(far)
    red_f1b.go()
    red_f2b.go()
    column_grad(n1, gpk, gq, 2, 2)
    red_qb = reduction("q_b", gq.at[1], order_of("yhl"), "came_q_")
    red_qb.go()
    red_f1a.go()
    column_grad(n1, gpk, gq, 0, 2)
    red_qa = reduction("q_a", gq.at[0], order_of("lyh"), "came_q_")
    red_qa.go()
    red_f2b.go()
    finish(third, grad=False)
    o_far = mv.remote(outp.at[3], outr.at[1], me.over_core)
    red_f1b.go()
    row_grad(ctx, d.at[c], r["d_send"], 0, 512, width // 512)
    d_swap = mv.remote(r["d_send"], d.at[c], me.over_core)
    o_far.wait_recv()
    finish(second, grad=False, plus=(outr.at[pl.ds(1, 1)],))
    o_x = mv.remote(outp.at[2], outx, me.over_x)
    d_swap.wait_recv()
    red_d = reduction("d", d, order_of("ylh"), "came_d")
    red_d.go()
    row_grad(act, f2a.at[c], f2a_s, 0, 512, width // 1024)
    f2a_swap = mv.remote(f2a_s, f2a.at[c], me.over_core)
    red_qb.go()
    red_f1a.go()
    f2a_swap.wait_recv()
    red_f2a = reduction("f2a", f2a, order_of("ylh"), "came_f2")
    red_f2a.go()
    finish(third, out=False)
    u_far = mv.remote(up.at[3], ur.at[1], me.over_core)
    red_d.go()
    u_far.wait_recv()
    finish(second, out=False, plus=(ur.at[pl.ds(1, 1)],))
    u_x = mv.remote(up.at[2], ux, me.over_x)
    red_qa.go()
    finish(near)
    u_near = mv.remote(up.at[1], ur.at[0], me.over_core)
    o_near = mv.remote(outp.at[1], outr.at[0], me.over_core)
    red_f2a.go()
    red_qb.go()

    def add_small(usum_v, qsum_v, fsum_v):
        for one in [mv.local(usum, usum_v), mv.local(qsum, qsum_v), mv.local(fsum, fsum_v)]:
            one.wait()
        acc[0, 0:4, :] = jnp.sum(usum_v[:, 0:4, :] + usum_v[:, 8:12, :], axis=0)
        for g in range(3):
            acc[0, 5 + g : 6 + g, ds((2 * s + c) * quarter, quarter)] = jnp.sum(
                qsum_v[:, 0:1, pl.ds(g * quarter, quarter)], axis=0
            )
        f_row = jnp.sum(fsum_v[:, 0:1, :] + fsum_v[:, 8:9, :], axis=0)
        acc[0, 8:9, ds(c * ffq, ffq)] = jnp.where(s == 0, f_row, 0.0)
        acc[0, 9:10, ds(c * ffq, ffq)] = jnp.where(s == 0, 0.0, f_row)

    pl.run_scoped(
        add_small,
        pltpu.VMEM((4, 16, width), F32),
        pltpu.VMEM((4, 8, 3 * quarter), F32),
        pltpu.VMEM((4, 16, ffq), F32),
    )
    bits_in_turn = (0,) + tuple(reversed(range(1, nbits)))
    small_peers = [me.over_core] + [me.over_bit(b) for b in bits_in_turn] + [me.over_x]
    small_step = [0, None]

    def small_go():
        k, flying = small_step
        if k > len(small_peers):
            return
        if flying is not None:
            flying.wait_recv()
            acc[k] = acc[k - 1] + got[k - 1]
        if k < len(small_peers):
            small_step[1] = mv.remote(acc.at[k], got.at[k], small_peers[k])
        else:
            r["tot"][...] = acc[k]
        small_step[0] = k + 1


    small_go()
    red_qa.go()
    small_go()
    red_d.go()
    red_f2a.go()


    for _ in range(nbits):
        for one in (red_f2a, red_f2b, red_f1a, red_f1b, red_qa, red_d, red_qb):
            if one.step < nbits:
                one.go()
    tok = lambda i: (i, 0)
    block = (rows // 8, width)

    def result_body(x, y, a, b, e, ua, ub, ue, stat, o, ou):
        xf = x[...].astype(F32)
        o[...] = (
            xf
            + (
                a[...].astype(F32)
                + b[...].astype(F32)
                + e[...].astype(F32)
                + (sm[:, pl.ds(7 * width + 4 * ffq, width)] + sm[:, pl.ds(8 * width + 4 * ffq, width)])
            )
        ).astype(BF)
        u = ua[...].astype(F32) + ub[...].astype(F32) + ue[...].astype(F32)
        mean, rstd = stat[:, 0:1], stat[:, 1:2]
        n = (xf - mean) * rstd
        ou[...] = y[...].astype(F32) + rstd * (
            u - jnp.mean(u, axis=1, keepdims=True) - n * jnp.mean(u * n, axis=1, keepdims=True)
        )

    last = []

    def hand_over(e, got):
        last.append(mv.remote(e.at[s, 1 - c], got.at[0], me.over_core))
        last.append(mv.remote(e.at[1 - s, c], got.at[1], me.over_x))
        last.append(mv.remote(e.at[1 - s, 1 - c], got.at[2], me.diagonal))

    e_f1, e_q, r_f1, r_q = r["e_f1"], r["e_q"], r["r_f1"], r["r_q"]

    def owners(end_f, end_q, o_f1, o_q, o_f2, o_d):
        before = len(mv.sent)
        for k, red in enumerate((red_f1a, red_f1b)):
            red.end(end_f)
            e_f1[k] = end_f[...].reshape(e_f1.shape[1:])
        hand_over(e_f1, r_f1)
        arrived([o_near, u_near, o_x, u_x])
        pipe(
            result_body,
            (8,),
            [
                (v, block, tok)
                for v in (hid, cot, outp.at[0], outr.at[0], outx, up.at[0], ur.at[0], ux)
            ]
            + [(st.at[0], (rows // 8, 128), tok)],
            [(r["result"], block, tok), (r["grad"], block, tok)],
        )
        small_go()
        for k, red in ((1, red_qb), (0, red_qa)):
            red.end(end_q)
            e_q[k] = end_q[...].reshape(e_q.shape[1:])
        hand_over(e_q, r_q)
        small_go()
        places = ((s, c), (s, 1 - c), (1 - s, c), (1 - s, 1 - c))
        arrived(last[:3])
        for k, (ps, pc) in enumerate(places):
            part = e_f1[s, c] if k == 0 else r_f1[k - 1]
            o_f1[:, ds((2 * ps + pc) * ffq, ffq)] = part.astype(F32)
        out = [mv.local(o_f1, r["o_f1"])]
        red_f2b.end(o_f2.at[:, pl.ds(half, half)])
        red_d.end(o_d)
        out.append(mv.local(o_d, r["o_d"]))
        small_go()
        red_f2a.end(o_f2.at[:, pl.ds(0, half)])
        out.append(mv.local(o_f2, r["o_f2"]))
        arrived(last[3:])
        for k, (ps, pc) in enumerate(places):
            for g in range(3):
                cols = pl.ds(g * quarter, quarter)
                part = e_q[s, c, :, cols] if k == 0 else r_q[k - 1, :, cols]
                o_q[:, ds(g * width + (2 * ps + pc) * quarter, quarter)] = part.astype(F32)
        out.append(mv.local(o_q, r["o_q"]))
        for _ in range(nbits + 3):
            small_go()
        for one in out:
            one.wait()
        for one in mv.sent[before:]:
            one.wait_send()
        del mv.sent[before:]

    pl.run_scoped(
        owners,
        pltpu.VMEM(g1.shape[-2:], BF),
        pltpu.VMEM(gq.shape[-2:], BF),
        pltpu.VMEM(r["o_f1"].shape, F32),
        pltpu.VMEM(r["o_q"].shape, F32),
        pltpu.VMEM(r["o_f2"].shape, F32),
        pltpu.VMEM(r["o_d"].shape, F32),
    )
    mv.finish()


def step(nbits, hid, cot, tab, small, wqkv, wdense, wfc1, wfc2):
    rows, width = hid.shape
    half, ff = wfc1.shape
    quarter, ffq = width // 4, ff // 4
    groups = 2**nbits
    own_rows = half // groups
    half_own = own_rows // 2
    per_ff = ffq // groups
    length = small.shape[1]
    bits = (2,) * nbits
    hbm, vmem = pl.BlockSpec(memory_space=pl.ANY), pl.BlockSpec(memory_space=pltpu.VMEM)
    sds = jax.ShapeDtypeStruct
    outs = {
        "result": (hbm, (rows, width), BF),
        "grad": (hbm, (rows, width), F32),
        "o_f2": (hbm, (per_ff, width), F32),
        "o_d": (hbm, (half_own, width), F32),
        "o_f1": (hbm, (half_own, ff), F32),
        "o_q": (hbm, (half_own, 3 * width), F32),
        "tot": (vmem, (16, width), F32),
        "xall": (hbm, (4, rows, width), BF),
        "call": (hbm, (4, rows, width), BF),
        "tall": (hbm, (4, rows, 128), F32),
        "n1": (hbm, (4, rows, width), BF),
        "n2": (hbm, (4, rows, width), BF),
        "st": (hbm, (4, rows, 128), F32),
        "gctx": (hbm, (4, rows, quarter), BF),
        "gact": (hbm, (4, rows, ffq), F32),
        "act": (hbm, (4, rows, ffq), BF),
        "gpre": (hbm, (4, rows, ffq), BF),
        "fsum": (hbm, (4, 16, ffq), F32),
        "ctx": (hbm, (4, rows, quarter), BF),
        "gpk": (hbm, (4, rows, 3 * quarter), BF),
        "qsum": (hbm, (4, 8, 3 * quarter), F32),
        "f2a": (hbm, bits + (per_ff, half), BF),
        "f2b": (hbm, bits + (per_ff, half), BF),
        "f2a_send": (hbm, bits[1:] + (per_ff, half), BF),
        "f2b_send": (hbm, bits[1:] + (per_ff, half), BF),
        "g1": (hbm, (2,) + bits + (own_rows, ffq), BF),
        "d": (hbm, bits + (half_own, width), BF),
        "d_send": (hbm, bits[1:] + (half_own, width), BF),
        "gq": (hbm, (2,) + bits + (own_rows, 3 * quarter), BF),
        "outp": (hbm, (4, rows, width), BF),
        "outr": (hbm, (2, rows, width), BF),
        "outx": (hbm, (rows, width), BF),
        "up": (hbm, (4, rows, width), BF),
        "ur": (hbm, (2, rows, width), BF),
        "ux": (hbm, (rows, width), BF),
        "usum": (hbm, (4, 16, width), F32),
    }
    extra = {}
    for name, tail in (
        ("f2a", (per_ff, half)),
        ("f2b", (per_ff, half)),
        ("f1a", (own_rows, ffq)),
        ("f1b", (own_rows, ffq)),
        ("d", (half_own, width)),
        ("q_a", (own_rows, 3 * quarter)),
        ("q_b", (own_rows, 3 * quarter)),
    ):
        for t in range(nbits):
            dims = (2,) * (nbits - 1 - t) + tail
            if t == 0:
                outs[f"{name}_got{t}"] = (hbm, dims, BF)
            else:
                extra[f"{name}_got{t}"] = pltpu.VMEM(dims, BF)
            if t == 1:
                extra[f"came_{name[:2]}"] = pltpu.VMEM(dims, BF)
            if t > 0:
                extra[f"{name}_sum{t}"] = pltpu.VMEM(dims, BF)
        for t in range(2, nbits + 1):
            dims = (2,) * max(nbits - 1 - t, 0) + tail
            extra[f"{name}_ahead{t}"] = pltpu.VMEM((2,) + dims, BF)
    scratch = {
        "wq": pltpu.VMEM((2,) + bits + (own_rows, 3 * quarter), BF),
        "wf1": pltpu.VMEM((2,) + bits + (own_rows, ffq), BF),
        "wf2": pltpu.VMEM((ffq, width), BF),
        "wd": pltpu.VMEM((quarter, width), BF),
        "sm_own": pltpu.VMEM((1, length), F32),
        "sm_got": pltpu.VMEM((1, length), F32),
        "sm": pltpu.VMEM((1, 2 * length), F32),
        "packed": pltpu.VMEM((rows, 3 * quarter), F32),
        "acc_k": pltpu.VMEM((rows, HEAD), F32),
        "acc_v": pltpu.VMEM((rows, HEAD), F32),
        "acc": pltpu.VMEM((3 + nbits, 16, width), F32),
        "got": pltpu.VMEM((2 + nbits, 16, width), F32),
        "r_f1": pltpu.VMEM((3, half_own, ffq), BF),
        "r_q": pltpu.VMEM((3, half_own, 3 * quarter), BF),
        "e_f1": pltpu.VMEM((2, 2, half_own, ffq), BF),
        "e_q": pltpu.VMEM((2, 2, half_own, 3 * quarter), BF),
        "send": pltpu.SemaphoreType.DMA((36 + 12 * nbits,)),
        "recv": pltpu.SemaphoreType.DMA((36 + 12 * nbits,)),
        "lsem": pltpu.SemaphoreType.DMA((40 + 14 * nbits,)),
        **extra,
    }
    ins = ("hid", "cot", "tab", "small", "wqkv", "wdense", "wfc1", "wfc2")
    got = pl.pallas_call(
        partial(step_kernel, nbits, ins + tuple(outs) + tuple(scratch)),
        in_specs=[hbm] * len(ins),
        out_specs=[one[0] for one in outs.values()],
        out_shape=[sds(*one[1:]) for one in outs.values()],
        scratch_shapes=list(scratch.values()),
        compiler_params=pltpu.CompilerParams(
            collective_id=0, has_side_effects=True, vmem_limit_bytes=VMEM_LIMIT
        ),
        name="step",
    )(
        hid,
        cot,
        tab,
        small,
        wqkv.reshape(bits + (own_rows, 3 * width)),
        wdense,
        wfc1.reshape(bits + (own_rows, ff)),
        wfc2,
    )
    return got[:7]


def rotary_table(seg):
    rows = seg.shape[0]
    index = jnp.arange(rows, dtype=jnp.int32)
    same = seg[:, None] == seg[None, :]
    first = jnp.min(jnp.where(same, index[None, :], rows), axis=1)
    offset = (index - first).astype(F32)
    frequency = jnp.exp(-jnp.log(10000.0) * jnp.arange(0, ROT, 2).astype(F32) / ROT)
    angles = offset[:, None] * frequency[None, :]
    ids = jnp.broadcast_to(seg.astype(F32)[:, None], (rows, 128 - ROT))
    return jnp.concatenate([jnp.cos(angles), jnp.sin(angles), ids], axis=1)


def local(
    nbits,
    hidden_in,
    out_cotangent,
    segment_ids,
    ln1_gain,
    ln1_bias,
    qkv_weight,
    qkv_bias,
    dense_weight,
    dense_bias,
    ln2_gain,
    ln2_bias,
    fc1_weight,
    fc1_bias,
    fc2_weight,
    fc2_bias,
):
    me = lax.axis_index("shard") * 2 ** (nbits + 1) + lax.axis_index("replica")
    owners = 2 ** (nbits + 2)
    width = hidden_in.shape[1]
    vectors = (
        ln1_gain, ln1_bias, ln2_gain, ln2_bias, qkv_bias, fc1_bias, dense_bias, fc2_bias
    )
    length = sum(v.shape[0] for v in vectors)
    small, lo = 0.0, 0
    for v in vectors:
        n = v.shape[0]
        small = small + jnp.pad(v.astype(F32), (lo, length - lo - n))
        lo += n
    result, grad, o_f2, o_d, o_f1, o_q, tot = step(
        nbits,
        hidden_in,
        out_cotangent,
        rotary_table(segment_ids),
        small[None],
        qkv_weight,
        dense_weight,
        fc1_weight,
        fc2_weight,
    )

    def own(v):
        return lax.dynamic_index_in_dim(v.reshape(v.shape[:-1] + (owners, -1)), me, v.ndim - 1, False)

    five = own(tot[:5])
    b_qkv = own(tot[5:8].reshape(-1))
    b_fc1 = own(tot[8:10].reshape(-1))
    return (
        result, grad, five[0], five[1], o_q, b_qkv, o_d, five[4],
        five[2], five[3], o_f1, b_fc1, o_f2, five[4],
    )


def solution(mesh):
    both = ("shard", "replica")
    nbits = (mesh.shape["replica"] // 2).bit_length() - 1
    wide, token, vector, matrix = P(both, None), P(both), P("shard"), P("shard", None)
    return jax.shard_map(
        partial(local, nbits),
        mesh=mesh,
        in_specs=(wide, wide, token, vector, vector, matrix, vector, matrix, vector)
        + (vector, vector, matrix, vector, matrix, vector),
        out_specs=(wide, wide, token, token, wide, token, wide, token)
        + (token, token, wide, token, wide, token),
        check_vma=False,
    )
```
